32 devices in a mesh: dp: 1 (over z), tp: 4 (over y), dm: 8 (over x, core).
Axes of the slice: x: 4, y: 4, z: 1, core: 2. Of those that a mesh axis runs over, the one named last changes fastest.
The devices are a block of a 4x4x8 slice.
Arguments:
- x_in: bfloat16 [2048, 5120], P('dp', 'dm')
- positions: int32 [2048], P(('dp', 'dm'))
- k_cache: bfloat16 [2048, 8, 64, 160], P(('dp', 'dm'), 'tp')
- v_cache: bfloat16 [2048, 8, 64, 160], P(('dp', 'dm'), 'tp')
- ln_gain: bfloat16 [5120], P('dm')
- w_q: bfloat16 [5120, 5120], P('dm', 'tp')
- w_k: bfloat16 [5120, 1280], P('dm', 'tp')
- w_v: bfloat16 [5120, 1280], P('dm', 'tp')
- w_gate: bfloat16 [5120, 13824], P('dm', 'tp')
- w_up: bfloat16 [5120, 13824], P('dm', 'tp')
- q_gain: bfloat16 [32, 160], P('tp')
- k_gain: bfloat16 [8, 160], P('tp')
- w_out: bfloat16 [5120, 5120], P('tp', 'dm')
- w_down: bfloat16 [13824, 5120], P('tp', 'dm')
Outputs:
- output 1: bfloat16 [2048, 5120], P('dp', 'dm')
- output 2: bfloat16 [2048, 8, 160], P(('dp', 'dm'), 'tp')
- output 3: bfloat16 [2048, 8, 160], P(('dp', 'dm'), 'tp')
All inputs are finite; a program needn't handle non-finite values.
Results may differ from the reference program's by a relative error of at most 0.0139342.
Values are sent between devices in bfloat16 or wider.
A program may use at most 768 MiB of HBM per device.

```python
import jax
import jax.numpy as jnp
from jax import lax

D = 5120
HEADS = 32
KV_HEADS = 8
HEAD = 160
FF = 13824
CTX = 64
BATCH = 2048
ROW_BLOCK = 8
NORM_EPS = 1e-5
ROPE_THETA = 75000000.0


def setup_inputs(seed: int = 0, part: int = 0) -> dict:
    part_keys = jax.random.split(jax.random.fold_in(jax.random.key(seed), part), 7)
    shared_keys = jax.random.split(jax.random.key(seed + 1), 10)
    col_pos = jnp.arange(D, dtype=jnp.float32) / D
    row_mu = jax.random.normal(part_keys[0], (BATCH, 1), jnp.float32)
    row_sd = jax.random.uniform(part_keys[1], (BATCH, 1), jnp.float32, 0.5, 1.5)
    col_off = 1.5 * (col_pos - 0.5)
    col_sd = 0.5 + col_pos
    x_noise = jax.random.normal(part_keys[2], (BATCH, D), jnp.float32)
    x_in = (row_mu + col_off[None, :] + row_sd * col_sd[None, :] * x_noise).astype(jnp.bfloat16)
    row_ids = jnp.arange(BATCH)
    pos_draw = jax.random.randint(part_keys[3], (BATCH,), 1, CTX + 1)
    positions = jnp.where(row_ids == 0, CTX, jnp.where(row_ids == 1, 1, pos_draw)).astype(jnp.int32)
    k_cache = (2.0 * jax.random.normal(part_keys[4], (BATCH, KV_HEADS, CTX, HEAD), jnp.float32)).astype(jnp.bfloat16)
    v_mean = jax.random.normal(part_keys[5], (BATCH, KV_HEADS, 1, HEAD), jnp.float32)
    v_cache = (0.6 * v_mean + jax.random.normal(part_keys[6], (BATCH, KV_HEADS, CTX, HEAD), jnp.float32)).astype(jnp.bfloat16)

    def normal_weight(key_w, fan_in, fan_out):
        return (jax.random.normal(key_w, (fan_in, fan_out), jnp.float32) * fan_in ** -0.5).astype(jnp.bfloat16)

    def gain_draw(key_g, shape_g):
        return (1.0 + 0.5 * jax.random.normal(key_g, shape_g, jnp.float32)).astype(jnp.bfloat16)

    return {
        'x_in': x_in,
        'positions': positions,
        'k_cache': k_cache,
        'v_cache': v_cache,
        'ln_gain': gain_draw(shared_keys[0], (D,)),
        'w_q': normal_weight(shared_keys[1], D, HEADS * HEAD),
        'w_k': normal_weight(shared_keys[2], D, KV_HEADS * HEAD),
        'w_v': normal_weight(shared_keys[3], D, KV_HEADS * HEAD),
        'w_gate': normal_weight(shared_keys[4], D, FF),
        'w_up': normal_weight(shared_keys[5], D, FF),
        'q_gain': gain_draw(shared_keys[6], (HEADS, HEAD)),
        'k_gain': gain_draw(shared_keys[7], (KV_HEADS, HEAD)),
        'w_out': normal_weight(shared_keys[8], HEADS * HEAD, D),
        'w_down': normal_weight(shared_keys[9], FF, D),
    }


def layer_norm_last(values, gain_w):
    centred = values - jnp.mean(values, axis=-1, keepdims=True)
    spread = jnp.mean(centred * centred, axis=-1, keepdims=True)
    return centred * lax.rsqrt(spread + NORM_EPS) * gain_w


def rotary(values, positions):
    inv_freq = ROPE_THETA ** (-jnp.arange(0, HEAD, 2, dtype=jnp.float32) / HEAD)
    angles = positions.astype(jnp.float32)[:, None] * inv_freq[None, :]
    cos_a = jnp.cos(angles)[:, None, :]
    sin_a = jnp.sin(angles)[:, None, :]
    pair_view = values.reshape(values.shape[:-1] + (HEAD // 2, 2))
    even_part = pair_view[..., 0]
    odd_part = pair_view[..., 1]
    turned = jnp.stack([even_part * cos_a - odd_part * sin_a, odd_part * cos_a + even_part * sin_a], axis=-1)
    return turned.reshape(values.shape)


def attend_rows(block_args):
    q_rot, k_new_rows, v_new_rows, k_old, v_old, pos_rows = block_args
    score_scale = HEAD ** -0.5
    q_f32 = q_rot.astype(jnp.float32)
    s_cache = jnp.einsum('rkgd,rksd->rkgs', q_f32, k_old.astype(jnp.float32)) * score_scale
    key_valid = jnp.arange(CTX)[None, None, None, :] < pos_rows[:, None, None, None]
    s_cache = jnp.where(key_valid, s_cache, -1e30)
    s_new = jnp.einsum('rkgd,rkd->rkg', q_f32, k_new_rows.astype(jnp.float32)) * score_scale
    row_max = jnp.maximum(jnp.max(s_cache, axis=-1), s_new)
    p_cache = jnp.exp(s_cache - row_max[..., None])
    p_new = jnp.exp(s_new - row_max)
    denom_sum = jnp.sum(p_cache, axis=-1) + p_new
    numer_acc = jnp.einsum('rkgs,rksd->rkgd', p_cache.astype(jnp.bfloat16).astype(jnp.float32), v_old.astype(jnp.float32))
    numer_acc = numer_acc + p_new[..., None] * v_new_rows.astype(jnp.float32)[:, :, None, :]
    return (numer_acc / denom_sum[..., None]).astype(jnp.bfloat16)


def reference(x_in, positions, k_cache, v_cache, ln_gain, w_q, w_k, w_v, w_gate, w_up, q_gain, k_gain, w_out, w_down):
    x_f32 = x_in.astype(jnp.float32)
    normed = layer_norm_last(x_f32, ln_gain.astype(jnp.float32)).astype(jnp.bfloat16)
    q_all = jnp.dot(normed, w_q, preferred_element_type=jnp.float32).astype(jnp.bfloat16)
    k_all = jnp.dot(normed, w_k, preferred_element_type=jnp.float32).astype(jnp.bfloat16)
    v_all = jnp.dot(normed, w_v, preferred_element_type=jnp.float32).astype(jnp.bfloat16)
    g_all = jnp.dot(normed, w_gate, preferred_element_type=jnp.float32).astype(jnp.bfloat16)
    u_all = jnp.dot(normed, w_up, preferred_element_type=jnp.float32).astype(jnp.bfloat16)
    q_per_kv = HEADS // KV_HEADS
    q_heads = layer_norm_last(q_all.reshape(BATCH, HEADS, HEAD).astype(jnp.float32), q_gain.astype(jnp.float32))
    q_rot = rotary(q_heads, positions).astype(jnp.bfloat16).reshape(BATCH, KV_HEADS, q_per_kv, HEAD)
    k_heads = layer_norm_last(k_all.reshape(BATCH, KV_HEADS, HEAD).astype(jnp.float32), k_gain.astype(jnp.float32))
    k_new = rotary(k_heads, positions).astype(jnp.bfloat16)
    v_new = v_all.reshape(BATCH, KV_HEADS, HEAD)
    num_blocks = BATCH // ROW_BLOCK

    def blocked(array_in):
        return array_in.reshape((num_blocks, ROW_BLOCK) + array_in.shape[1:])

    attn_rows = lax.map(attend_rows, (blocked(q_rot), blocked(k_new), blocked(v_new), blocked(k_cache), blocked(v_cache), blocked(positions)))
    attn_flat = attn_rows.reshape(BATCH, HEADS * HEAD)
    mlp_act = (jax.nn.silu(g_all.astype(jnp.float32)) * u_all.astype(jnp.float32)).astype(jnp.bfloat16)
    branch_sum = jnp.dot(attn_flat, w_out, preferred_element_type=jnp.float32) + jnp.dot(mlp_act, w_down, preferred_element_type=jnp.float32)
    x_out = (x_f32 + branch_sum).astype(jnp.bfloat16)
    return (x_out, k_new, v_new)
```

```python
import functools

import jax
import jax.numpy as jnp
from jax import lax
from jax.experimental import pallas as pl
from jax.experimental.pallas import tpu as pltpu
from jax.sharding import PartitionSpec as P

NORM_EPS = 1e-5
ROPE_THETA = 75000000.0
MESH = pl.DeviceIdType.MESH
BF16 = jnp.bfloat16
F32 = jnp.float32
ANY = pl.ANY
VMEM_LIMIT = 66 * 1024 * 1000 - 1024 * 600


def layer_norm_last(values, gain_w):
    centred = values - jnp.mean(values, axis=-1, keepdims=True)
    spread = jnp.mean(centred * centred, axis=-1, keepdims=True)
    return centred * lax.rsqrt(spread + NORM_EPS) * gain_w


def rotary(values, positions):
    head_dim = values.shape[-1]
    inv_freq = ROPE_THETA ** (-jnp.arange(0, head_dim, 2, dtype=jnp.float32) / head_dim)
    angles = positions.astype(jnp.float32)[:, None] * inv_freq[None, :]
    cos_a = jnp.cos(angles)[:, None, :]
    sin_a = jnp.sin(angles)[:, None, :]
    pair_view = values.reshape(values.shape[:-1] + (head_dim // 2, 2))
    even_part = pair_view[..., 0]
    odd_part = pair_view[..., 1]
    turned = jnp.stack([even_part * cos_a - odd_part * sin_a, odd_part * cos_a + even_part * sin_a], axis=-1)
    return turned.reshape(values.shape)


def project_kernel(nx, ntile, x_ref, wq_ref, wk_ref, wv_ref, wg_ref, wu_ref,
                   q_out, k_out, v_out, act_out,
                   xbuf, bq, bk, bv, bg, bu, rq, rk, rg, lq, lv, lu,
                   x_loc, x_snd, x_rcv, w_loc, w_snd, w_rcv, r_snd, r_rcv):
    dm = lax.axis_index('dm')
    xi = dm // 2
    core = lax.rem(dm, 2)
    other = 2 * xi + 1 - core
    right = lax.rem(xi + 1, nx) * 2 + core
    left = lax.rem(xi + nx - 1, nx) * 2 + core
    rb = xbuf.shape[1]
    hid = x_ref.shape[1]
    tw = wg_ref.shape[1] // ntile

    pieces = [(wq_ref, bq, None), (wk_ref, bk, None), (wv_ref, bv, None)]
    for t in range(ntile):
        pieces.append((wg_ref, bg, pl.ds(t * tw, tw)))
        pieces.append((wu_ref, bu, pl.ds(t * tw, tw)))

    def x_local(j):
        return pltpu.make_async_copy(
            x_ref.at[pl.ds((2 * j + core) * rb, rb), :], xbuf.at[j, :, pl.ds(0, hid)], x_loc.at[j])

    def x_remote(j):
        return pltpu.make_async_remote_copy(
            src_ref=x_ref.at[pl.ds((2 * j + 1 - core) * rb, rb), :], dst_ref=xbuf.at[j, :, pl.ds(hid, hid)],
            send_sem=x_snd.at[j], recv_sem=x_rcv.at[j], device_id={'dm': other}, device_id_type=MESH)

    def w_local(n):
        src, dst, cols = pieces[n]
        if cols is None:
            return pltpu.make_async_copy(src, dst.at[pl.ds(0, hid), :], w_loc.at[n])
        return pltpu.make_async_copy(src.at[:, cols], dst.at[pl.ds(0, hid), cols], w_loc.at[n])

    def w_remote(n):
        src, dst, cols = pieces[n]
        if cols is not None:
            src = src.at[:, cols]
            dst = dst.at[pl.ds(hid, hid), cols]
        else:
            dst = dst.at[pl.ds(hid, hid), :]
        return pltpu.make_async_remote_copy(
            src_ref=src, dst_ref=dst, send_sem=w_snd.at[n], recv_sem=w_rcv.at[n],
            device_id={'dm': other}, device_id_type=MESH)

    barrier = pltpu.get_barrier_semaphore()
    for peer in (other, right, left):
        pl.semaphore_signal(barrier, inc=1, device_id={'dm': peer}, device_id_type=MESH)
    pl.semaphore_wait(barrier, 3)

    for j in range(nx):
        x_local(j).start()
        x_remote(j).start()
    for n in range(len(pieces)):
        w_local(n).start()
        w_remote(n).start()

    for ref in (rq, rk, rg, lq, lv, lu):
        ref[0] = jnp.zeros(ref.shape[1:], ref.dtype)

    for j in range(nx):
        x_local(j).wait()
        x_remote(j).wait()

    def hop(d, t, s, slot, cols):
        nxt = jnp.minimum(s + 1, nx - 1)
        return pltpu.make_async_remote_copy(
            src_ref=slot.at[s, :, cols], dst_ref=slot.at[nxt, :, cols],
            send_sem=r_snd.at[d, t, s], recv_sem=r_rcv.at[d, t, nxt],
            device_id={'dm': left if d else right}, device_id_type=MESH)

    def arrived(d, t, s, slot, cols):
        return pltpu.make_async_remote_copy(
            src_ref=slot.at[s, :, cols], dst_ref=slot.at[s, :, cols],
            send_sem=r_snd.at[d, t, s], recv_sem=r_rcv.at[d, t, s],
            device_id={'dm': left if d else right}, device_id_type=MESH)

    def tile(d, t, s, weight, w_cols, slot, cols):
        row = lax.rem(xi + 1 + s, nx) if d else lax.rem(xi + 2 * nx - 1 - s, nx)
        part = jnp.dot(xbuf[row], weight[:, w_cols], preferred_element_type=F32)

        @pl.when(s > 0)
        def _():
            arrived(d, t, s, slot, cols).wait_recv()

        slot[s, :, cols] = (part + slot[s, :, cols].astype(F32)).astype(BF16)

        @pl.when(s < nx - 1)
        def _():
            hop(d, t, s, slot, cols).start()

    def wait_piece(n):
        w_local(n).wait()
        w_remote(n).wait()

    half = rq.shape[2]
    kw = rk.shape[2]

    def step(s, carry):
        @pl.when(s == 0)
        def _():
            wait_piece(0)

        tile(0, 0, s, bq, pl.ds(0, half), rq, pl.ds(0, half))
        tile(1, 0, s, bq, pl.ds(half, half), lq, pl.ds(0, half))

        @pl.when(s == 0)
        def _():
            wait_piece(1)
            wait_piece(2)

        tile(0, 1, s, bk, pl.ds(0, kw), rk, pl.ds(0, kw))
        tile(1, 1, s, bv, pl.ds(0, kw), lv, pl.ds(0, kw))
        for t in range(ntile):
            @pl.when(s == 0)
            def _():
                wait_piece(3 + 2 * t)
                wait_piece(4 + 2 * t)

        def mlp(t, inner):
            cols = pl.ds(pl.multiple_of(t * tw, 128), tw)
            tile(0, 2 + t, s, bg, cols, rg, cols)
            tile(1, 2 + t, s, bu, cols, lu, cols)

            @pl.when(s == nx - 1)
            def _():
                gate = rg[nx - 1, :, cols].astype(F32)
                up = lu[nx - 1, :, cols].astype(F32)
                act_out[:, cols] = (gate / (1.0 + jnp.exp(-gate)) * up).astype(BF16)

            return inner

        return lax.fori_loop(0, ntile, mlp, carry)

    lax.fori_loop(0, nx, step, 0)
    q_out[:, :half] = rq[nx - 1]
    q_out[:, half:] = lq[nx - 1]
    k_out[...] = rk[nx - 1]
    v_out[...] = lv[nx - 1]

    def sent(s, carry):
        hop(0, 0, s, rq, pl.ds(0, half)).wait_send()
        hop(1, 0, s, lq, pl.ds(0, half)).wait_send()
        hop(0, 1, s, rk, pl.ds(0, kw)).wait_send()
        hop(1, 1, s, lv, pl.ds(0, kw)).wait_send()
        for t in range(ntile):
            cols = pl.ds(t * tw, tw)
            hop(0, 2 + t, s, rg, cols).wait_send()
            hop(1, 2 + t, s, lu, cols).wait_send()
        return carry

    lax.fori_loop(0, nx - 1, sent, 0)


def project(nx, h, w_q, w_k, w_v, w_gate, w_up):
    rows, hid = h.shape
    rb = rows // (2 * nx)
    nq, nk, nf = w_q.shape[1], w_k.shape[1], w_gate.shape[1]
    ntile = 3
    npiece = 3 + 2 * ntile
    vmem = pl.BlockSpec(memory_space=pltpu.VMEM)
    return pl.pallas_call(
        functools.partial(project_kernel, nx, ntile),
        out_shape=(jax.ShapeDtypeStruct((rb, nq), BF16), jax.ShapeDtypeStruct((rb, nk), BF16),
                   jax.ShapeDtypeStruct((rb, nk), BF16), jax.ShapeDtypeStruct((rb, nf), BF16)),
        in_specs=[pl.BlockSpec(memory_space=ANY)] * 6,
        out_specs=(vmem,) * 4,
        scratch_shapes=[
            pltpu.VMEM((nx, rb, 2 * hid), BF16),
            pltpu.VMEM((2 * hid, nq), BF16),
            pltpu.VMEM((2 * hid, nk), BF16),
            pltpu.VMEM((2 * hid, nk), BF16),
            pltpu.VMEM((2 * hid, nf), BF16),
            pltpu.VMEM((2 * hid, nf), BF16),
            pltpu.VMEM((nx, rb, nq // 2), BF16),
            pltpu.VMEM((nx, rb, nk), BF16),
            pltpu.VMEM((nx, rb, nf), BF16),
            pltpu.VMEM((nx, rb, nq // 2), BF16),
            pltpu.VMEM((nx, rb, nk), BF16),
            pltpu.VMEM((nx, rb, nf), BF16),
            pltpu.SemaphoreType.DMA((nx,)),
            pltpu.SemaphoreType.DMA((nx,)),
            pltpu.SemaphoreType.DMA((nx,)),
            pltpu.SemaphoreType.DMA((npiece,)),
            pltpu.SemaphoreType.DMA((npiece,)),
            pltpu.SemaphoreType.DMA((npiece,)),
            pltpu.SemaphoreType.DMA((2, 2 + ntile, nx)),
            pltpu.SemaphoreType.DMA((2, 2 + ntile, nx)),
        ],
        compiler_params=pltpu.CompilerParams(collective_id=0, has_side_effects=True, vmem_limit_bytes=VMEM_LIMIT),
        name='project',
    )(h, w_q, w_k, w_v, w_gate, w_up)


def attend(q_rot, k_rot, v_new, k_cache, v_cache, positions):
    score_scale = q_rot.shape[-1] ** -0.5
    s_cache = jnp.einsum('rkgd,rksd->rkgs', q_rot, k_cache, preferred_element_type=jnp.float32) * score_scale
    key_valid = jnp.arange(k_cache.shape[2])[None, None, None, :] < positions[:, None, None, None]
    s_cache = jnp.where(key_valid, s_cache, -1e30)
    s_new = jnp.einsum('rkgd,rkd->rkg', q_rot, k_rot, preferred_element_type=jnp.float32) * score_scale
    row_max = jnp.maximum(jnp.max(s_cache, axis=-1), s_new)
    p_cache = jnp.exp(s_cache - row_max[..., None])
    p_new = jnp.exp(s_new - row_max)
    denom_sum = jnp.sum(p_cache, axis=-1) + p_new
    numer_acc = jnp.einsum('rkgs,rksd->rkgd', p_cache.astype(jnp.bfloat16), v_cache, preferred_element_type=jnp.float32)
    numer_acc = numer_acc + p_new[..., None] * v_new.astype(jnp.float32)[:, :, None, :]
    return (numer_acc / denom_sum[..., None]).astype(jnp.bfloat16)


def solution(mesh):
    dm_size = mesh.shape['dm']
    nx = dm_size // 2
    x_spec = P('dp', 'dm')
    row_spec = P(('dp', 'dm'))
    cache_spec = P(('dp', 'dm'), 'tp', None, None)
    new_spec = P(('dp', 'dm'), 'tp', None)
    hid_tp = P('dm', 'tp')
    tp_hid = P('tp', 'dm')
    head_spec = P('tp', None)

    def device_step(x_in, positions, k_cache, v_cache, ln_gain, w_q, w_k, w_v, w_gate, w_up, q_gain, k_gain, w_out, w_down):
        rows_loc = k_cache.shape[0]
        kv_loc = k_cache.shape[1]
        head_dim = k_cache.shape[3]
        heads_loc = q_gain.shape[0]
        hid = x_in.shape[1]
        d_model = hid * dm_size
        x_f32 = x_in.astype(jnp.float32)
        loc_mean = jnp.mean(x_f32, axis=1)
        loc_cent = x_f32 - loc_mean[:, None]
        loc_m2 = jnp.sum(loc_cent * loc_cent, axis=1)
        stats = lax.all_gather(jnp.stack([loc_mean, loc_m2]), 'dm', axis=0)
        row_mean = jnp.mean(stats[:, 0], axis=0)
        diff = stats[:, 0] - row_mean[None]
        row_var = (jnp.sum(stats[:, 1], axis=0) + hid * jnp.sum(diff * diff, axis=0)) / d_model
        normed = ((x_f32 - row_mean[:, None]) * lax.rsqrt(row_var + NORM_EPS)[:, None] * ln_gain.astype(jnp.float32)).astype(jnp.bfloat16)
        q_rows, k_rows, v_rows, act = project(nx, normed, w_q, w_k, w_v, w_gate, w_up)
        q_heads = layer_norm_last(q_rows.reshape(rows_loc, heads_loc, head_dim).astype(jnp.float32), q_gain.astype(jnp.float32))
        q_rot = rotary(q_heads, positions).astype(jnp.bfloat16).reshape(rows_loc, kv_loc, heads_loc // kv_loc, head_dim)
        k_heads = layer_norm_last(k_rows.reshape(rows_loc, kv_loc, head_dim).astype(jnp.float32), k_gain.astype(jnp.float32))
        k_new = rotary(k_heads, positions).astype(jnp.bfloat16)
        v_new = v_rows.reshape(rows_loc, kv_loc, head_dim)
        attn_loc = attend(q_rot, k_new, v_new, k_cache, v_cache, positions).reshape(rows_loc, heads_loc * head_dim)
        act_all = lax.all_gather(act, 'dm', axis=0, tiled=True)
        attn_all = lax.all_gather(attn_loc, 'dm', axis=0, tiled=True)
        part_out = jnp.dot(attn_all, w_out, preferred_element_type=jnp.float32) + jnp.dot(act_all, w_down, preferred_element_type=jnp.float32)
        out_sum = lax.psum(part_out.astype(jnp.bfloat16), 'tp')
        x_out = (x_f32 + out_sum.astype(jnp.float32)).astype(jnp.bfloat16)
        return x_out, k_new, v_new

    return jax.shard_map(
        device_step,
        mesh=mesh,
        in_specs=(x_spec, row_spec, cache_spec, cache_spec, P('dm'), hid_tp, hid_tp, hid_tp, hid_tp, hid_tp, head_spec, head_spec, tp_hid, tp_hid),
        out_specs=(x_spec, new_spec, new_spec),
        check_vma=False,
    )
```

```python
import functools

import jax
import jax.numpy as jnp
from jax import lax
from jax.experimental import pallas as pl
from jax.experimental.pallas import tpu as pltpu
from jax.sharding import PartitionSpec as P

NORM_EPS = 1e-5
ROPE_THETA = 75000000.0
MESH = pl.DeviceIdType.MESH
BF16 = jnp.bfloat16
F32 = jnp.float32
ANY = pl.ANY
VMEM_LIMIT = 66 * 1024 * 1000 - 1024 * 600


def project_kernel(nx, ntile, x_ref, wq_ref, wk_ref, wv_ref, wg_ref, wu_ref,
                   qk_out, v_out, act_out,
                   xbuf, bq, bk, bv, bg, bu, rq, rk, rg, lq, lv, lu,
                   x_loc, x_snd, x_rcv, w_loc, w_snd, w_rcv, r_snd, r_rcv):
    dm = lax.axis_index('dm')
    xi = dm // 2
    core = lax.rem(dm, 2)
    other = 2 * xi + 1 - core
    right = lax.rem(xi + 1, nx) * 2 + core
    left = lax.rem(xi + nx - 1, nx) * 2 + core
    rb = xbuf.shape[1]
    hid = x_ref.shape[1]
    tw = wg_ref.shape[1] // ntile

    pieces = [(wq_ref, bq, None), (wk_ref, bk, None), (wv_ref, bv, None)]
    for t in range(ntile):
        pieces.append((wg_ref, bg, pl.ds(t * tw, tw)))
        pieces.append((wu_ref, bu, pl.ds(t * tw, tw)))

    def x_local(j):
        return pltpu.make_async_copy(
            x_ref.at[pl.ds((2 * j + core) * rb, rb), :], xbuf.at[j, :, pl.ds(0, hid)], x_loc.at[j])

    def x_remote(j):
        return pltpu.make_async_remote_copy(
            src_ref=x_ref.at[pl.ds((2 * j + 1 - core) * rb, rb), :], dst_ref=xbuf.at[j, :, pl.ds(hid, hid)],
            send_sem=x_snd.at[j], recv_sem=x_rcv.at[j], device_id={'dm': other}, device_id_type=MESH)

    def w_local(n):
        src, dst, cols = pieces[n]
        if cols is None:
            return pltpu.make_async_copy(src, dst.at[pl.ds(0, hid), :], w_loc.at[n])
        return pltpu.make_async_copy(src.at[:, cols], dst.at[pl.ds(0, hid), cols], w_loc.at[n])

    def w_remote(n):
        src, dst, cols = pieces[n]
        if cols is not None:
            src = src.at[:, cols]
            dst = dst.at[pl.ds(hid, hid), cols]
        else:
            dst = dst.at[pl.ds(hid, hid), :]
        return pltpu.make_async_remote_copy(
            src_ref=src, dst_ref=dst, send_sem=w_snd.at[n], recv_sem=w_rcv.at[n],
            device_id={'dm': other}, device_id_type=MESH)

    barrier = pltpu.get_barrier_semaphore()
    for peer in (other, right, left):
        pl.semaphore_signal(barrier, inc=1, device_id={'dm': peer}, device_id_type=MESH)
    pl.semaphore_wait(barrier, 3)

    for j in range(nx):
        x_local(j).start()
        x_remote(j).start()
    for n in range(len(pieces)):
        w_local(n).start()
        w_remote(n).start()

    for ref in (rq, rk, rg, lq, lv, lu):
        ref[0] = jnp.zeros(ref.shape[1:], ref.dtype)

    for j in range(nx):
        x_local(j).wait()
        x_remote(j).wait()

    def hop(d, t, s, slot, cols):
        nxt = jnp.minimum(s + 1, nx - 1)
        return pltpu.make_async_remote_copy(
            src_ref=slot.at[s, :, cols], dst_ref=slot.at[nxt, :, cols],
            send_sem=r_snd.at[d, t, s], recv_sem=r_rcv.at[d, t, nxt],
            device_id={'dm': left if d else right}, device_id_type=MESH)

    def arrived(d, t, s, slot, cols):
        return pltpu.make_async_remote_copy(
            src_ref=slot.at[s, :, cols], dst_ref=slot.at[s, :, cols],
            send_sem=r_snd.at[d, t, s], recv_sem=r_rcv.at[d, t, s],
            device_id={'dm': left if d else right}, device_id_type=MESH)

    def tile(d, t, s, weight, w_cols, slot, cols):
        row = lax.rem(xi + 1 + s, nx) if d else lax.rem(xi + 2 * nx - 1 - s, nx)
        part = jnp.dot(xbuf[row], weight[:, w_cols], preferred_element_type=F32)

        @pl.when(s > 0)
        def _():
            arrived(d, t, s, slot, cols).wait_recv()

        slot[s, :, cols] = (part + slot[s, :, cols].astype(F32)).astype(BF16)

        @pl.when(s < nx - 1)
        def _():
            hop(d, t, s, slot, cols).start()

    def wait_piece(n):
        w_local(n).wait()
        w_remote(n).wait()

    half = rq.shape[2]
    kw = rk.shape[2]

    def step(s, carry):
        @pl.when(s == 0)
        def _():
            wait_piece(0)

        tile(0, 0, s, bq, pl.ds(0, half), rq, pl.ds(0, half))
        tile(1, 0, s, bq, pl.ds(half, half), lq, pl.ds(0, half))

        @pl.when(s == 0)
        def _():
            wait_piece(1)
            wait_piece(2)

        tile(0, 1, s, bk, pl.ds(0, kw), rk, pl.ds(0, kw))
        tile(1, 1, s, bv, pl.ds(0, kw), lv, pl.ds(0, kw))
        for t in range(ntile):
            @pl.when(s == 0)
            def _():
                wait_piece(3 + 2 * t)
                wait_piece(4 + 2 * t)

        def mlp(t, inner):
            cols = pl.ds(pl.multiple_of(t * tw, 128), tw)
            tile(0, 2 + t, s, bg, cols, rg, cols)
            tile(1, 2 + t, s, bu, cols, lu, cols)

            @pl.when(s == nx - 1)
            def _():
                gate = rg[nx - 1, :, cols].astype(F32)
                up = lu[nx - 1, :, cols].astype(F32)
                act_out[:, cols] = (gate / (1.0 + jnp.exp(-gate)) * up).astype(BF16)

            return inner

        return lax.fori_loop(0, ntile, mlp, carry)

    lax.fori_loop(0, nx, step, 0)
    qk_out[:, :half] = rq[nx - 1]
    qk_out[:, half:2 * half] = lq[nx - 1]
    qk_out[:, 2 * half:2 * half + kw] = rk[nx - 1]
    qk_out[:, 2 * half + kw:] = jnp.zeros((rb, qk_out.shape[1] - 2 * half - kw), BF16)
    v_out[...] = lv[nx - 1]

    def sent(s, carry):
        hop(0, 0, s, rq, pl.ds(0, half)).wait_send()
        hop(1, 0, s, lq, pl.ds(0, half)).wait_send()
        hop(0, 1, s, rk, pl.ds(0, kw)).wait_send()
        hop(1, 1, s, lv, pl.ds(0, kw)).wait_send()
        for t in range(ntile):
            cols = pl.ds(t * tw, tw)
            hop(0, 2 + t, s, rg, cols).wait_send()
            hop(1, 2 + t, s, lu, cols).wait_send()
        return carry

    lax.fori_loop(0, nx - 1, sent, 0)


def project(nx, h, w_q, w_k, w_v, w_gate, w_up):
    rows, hid = h.shape
    rb = rows // (2 * nx)
    nq, nk, nf = w_q.shape[1], w_k.shape[1], w_gate.shape[1]
    ntile = 3
    npiece = 3 + 2 * ntile
    vmem = pl.BlockSpec(memory_space=pltpu.VMEM)
    return pl.pallas_call(
        functools.partial(project_kernel, nx, ntile),
        out_shape=(jax.ShapeDtypeStruct((rb, nq + pl.cdiv(nk, 128) * 128), BF16),
                   jax.ShapeDtypeStruct((rb, nk), BF16), jax.ShapeDtypeStruct((rb, nf), BF16)),
        in_specs=[pl.BlockSpec(memory_space=ANY)] * 6,
        out_specs=(vmem,) * 3,
        scratch_shapes=[
            pltpu.VMEM((nx, rb, 2 * hid), BF16),
            pltpu.VMEM((2 * hid, nq), BF16),
            pltpu.VMEM((2 * hid, nk), BF16),
            pltpu.VMEM((2 * hid, nk), BF16),
            pltpu.VMEM((2 * hid, nf), BF16),
            pltpu.VMEM((2 * hid, nf), BF16),
            pltpu.VMEM((nx, rb, nq // 2), BF16),
            pltpu.VMEM((nx, rb, nk), BF16),
            pltpu.VMEM((nx, rb, nf), BF16),
            pltpu.VMEM((nx, rb, nq // 2), BF16),
            pltpu.VMEM((nx, rb, nk), BF16),
            pltpu.VMEM((nx, rb, nf), BF16),
            pltpu.SemaphoreType.DMA((nx,)),
            pltpu.SemaphoreType.DMA((nx,)),
            pltpu.SemaphoreType.DMA((nx,)),
            pltpu.SemaphoreType.DMA((npiece,)),
            pltpu.SemaphoreType.DMA((npiece,)),
            pltpu.SemaphoreType.DMA((npiece,)),
            pltpu.SemaphoreType.DMA((2, 2 + ntile, nx)),
            pltpu.SemaphoreType.DMA((2, 2 + ntile, nx)),
        ],
        compiler_params=pltpu.CompilerParams(collective_id=0, has_side_effects=True, vmem_limit_bytes=VMEM_LIMIT),
        name='project',
    )(h, w_q, w_k, w_v, w_gate, w_up)


def swap_pairs(v):
    width = v.shape[-1]
    lane = lax.broadcasted_iota(jnp.int32, v.shape, v.ndim - 1)
    return jnp.where(lax.rem(lane, 2) == 0, pltpu.roll(v, width - 1, v.ndim - 1), pltpu.roll(v, 1, v.ndim - 1))


def finish_kernel(nx, ny, heads, kv_heads, act_ref, qk_ref, v_ref, kc_ref, vc_ref, hi_ref, cos_ref, sin_ref, gain_ref, gswap_ref,
                  wo_ref, wd_ref, x_ref, out_ref, k_out,
                  gath, w2, qb, kbuf, vbuf, pb, r1, mf, mq, r2,
                  c_loc, kv_loc, s_own, s_opp, s_par, recv, y1s, y1r, y2s, y2r, y3s, y3r, y4s, y4r):
    dm = lax.axis_index('dm')
    y = lax.axis_index('tp')
    xi = dm // 2
    core = lax.rem(dm, 2)
    other = 2 * xi + 1 - core
    right = lax.rem(xi + 1, nx) * 2 + core
    left = lax.rem(xi + nx - 1, nx) * 2 + core
    nf = act_ref.shape[1]
    rb = act_ref.shape[0]
    hb, qtr = rb // 2, rb // 4
    head = cos_ref.shape[1]
    natt = heads * head
    group = heads // kv_heads
    flip, mirror = y + 1 - 2 * lax.rem(y, 2), ny - 1 - y
    p1 = flip + core * (mirror - flip)
    p2 = mirror + core * (flip - mirror)
    bit_a, bit_b, bit_c = lax.rem((y + 1) // 2, 2), y // 2, lax.rem(y, 2)
    b1 = bit_a + core * (bit_b - bit_a)
    b2 = bit_b + core * (bit_c - bit_b)

    act_cols, att_cols = pl.ds(natt, nf), pl.ds(0, natt)

    def to(peer):
        return dict(device_id={'dm': peer}, device_id_type=MESH)

    def to_y(peer):
        return dict(device_id={'tp': peer}, device_id_type=MESH)

    def own_send(n, h, kind):
        peer, slot = ((right, 4), (left, 2), (other, 1))[n]
        cols = att_cols if kind else act_cols
        src = gath.at[0, pl.ds(h * hb, hb), cols] if kind else act_ref.at[pl.ds(h * hb, hb), :]
        return pltpu.make_async_remote_copy(
            src_ref=src, dst_ref=gath.at[slot, pl.ds(h * hb, hb), cols],
            send_sem=s_own.at[n, h, kind], recv_sem=recv.at[slot, h, kind], **to(peer))

    def opp_send(n, kind):
        peer, slot, h = ((right, 4, 0), (left, 2, 1))[n]
        cols = att_cols if kind else act_cols
        return pltpu.make_async_remote_copy(
            src_ref=gath.at[slot, pl.ds(h * hb, hb), cols], dst_ref=gath.at[6, pl.ds(h * hb, hb), cols],
            send_sem=s_opp.at[n, kind], recv_sem=recv.at[6, h, kind], **to(peer))

    def par_send(slot, h, kind):
        cols = att_cols if kind else act_cols
        return pltpu.make_async_remote_copy(
            src_ref=gath.at[slot, pl.ds(h * hb, hb), cols], dst_ref=gath.at[slot + 1, pl.ds(h * hb, hb), cols],
            send_sem=s_par.at[slot // 2 - 1, h, kind], recv_sem=recv.at[slot + 1, h, kind], **to(other))

    def landed(slot, h, kind):
        cols = att_cols if kind else act_cols
        part = gath.at[slot, pl.ds(h * hb, hb), cols]
        return pltpu.make_async_remote_copy(
            src_ref=part, dst_ref=part, send_sem=s_own.at[0, 0, 0], recv_sem=recv.at[slot, h, kind], **to(other))

    n_loc = 3
    locals_ = [pltpu.make_async_copy(act_ref, gath.at[0, :, act_cols], c_loc.at[0]),
               pltpu.make_async_copy(wo_ref, w2.at[att_cols, :], c_loc.at[1]),
               pltpu.make_async_copy(wd_ref, w2.at[act_cols, :], c_loc.at[2])]

    rg = kbuf.shape[1]
    n_groups = rb // rg

    def cache_copies(g, slot):
        rows = pl.ds(g * rg, rg)
        return (pltpu.make_async_copy(kc_ref.at[rows], kbuf.at[slot], kv_loc.at[0, slot]),
                pltpu.make_async_copy(vc_ref.at[rows], vbuf.at[slot], kv_loc.at[1, slot]))

    for copy in cache_copies(0, 0):
        copy.start()

    barrier = pltpu.get_barrier_semaphore()
    for peer in (other, right, left):
        pl.semaphore_signal(barrier, inc=1, **to(peer))
    for peer in (p1, p2):
        pl.semaphore_signal(barrier, inc=1, **to_y(peer))
    pl.semaphore_wait(barrier, 5)

    for h in range(2):
        for n in range(3):
            own_send(n, h, 0).start()
    for copy in locals_:
        copy.start()

    qk = qk_ref[...].astype(F32)
    qk_swap = swap_pairs(qk)
    cos_a, sin_a = cos_ref[...], sin_ref[...]
    for n in range(heads + kv_heads):
        one = qk[:, n * head:(n + 1) * head]
        two = qk_swap[:, n * head:(n + 1) * head]
        mean = jnp.mean(one, axis=-1, keepdims=True)
        centred = one - mean
        scale = lax.rsqrt(jnp.mean(centred * centred, axis=-1, keepdims=True) + NORM_EPS)
        turned = centred * scale * gain_ref[n:n + 1, :] * cos_a + (two - mean) * scale * gswap_ref[n:n + 1, :] * sin_a
        qb[n] = turned.astype(BF16)
        if n >= heads:
            k_out[n - heads] = turned.astype(BF16)

    ctx = kbuf.shape[3]
    score_scale = head ** -0.5
    wide = group * rg
    nt = (((1,), (1,)), ((), ()))
    tn = (((0,), (0,)), ((), ()))

    def attend_group(g, carry):
        slot = lax.rem(g, 2)
        for copy in cache_copies(g, slot):
            copy.wait()

        @pl.when(g < n_groups - 1)
        def _():
            for copy in cache_copies(g + 1, 1 - slot):
                copy.start()

        rows = pl.ds(pl.multiple_of(g * rg, rg), rg)
        col_row = lax.rem(lax.broadcasted_iota(jnp.int32, (1, wide), 1), rg)
        low = col_row * ctx
        high = hi_ref[g]
        for kv in range(kv_heads):
            q_cols = jnp.concatenate([qb[kv * group + j, rows, :] for j in range(group)], axis=0)
            keys = kbuf[slot, :, kv].reshape(rg * ctx, head)
            vals = vbuf[slot, :, kv].reshape(rg * ctx, head)
            k_one = qb[heads + kv, rows, :]
            v_one = v_ref[rows, kv * head:(kv + 1) * head]
            scores = lax.dot_general(keys, q_cols, nt, preferred_element_type=F32) * score_scale
            at = lax.broadcasted_iota(jnp.int32, scores.shape, 0)
            scores = jnp.where((at >= low) & (at < high), scores, -1e30)
            s_one = lax.dot_general(k_one, q_cols, nt, preferred_element_type=F32) * score_scale
            at_one = lax.broadcasted_iota(jnp.int32, s_one.shape, 0)
            s_one = jnp.where(at_one == col_row, s_one, -1e30)
            top = jnp.maximum(jnp.max(scores, axis=0, keepdims=True), jnp.max(s_one, axis=0, keepdims=True))
            probs = jnp.exp(scores - top)
            p_one = jnp.exp(s_one - top)
            denom = jnp.sum(probs, axis=0, keepdims=True) + jnp.sum(p_one, axis=0, keepdims=True)
            p_high = p_one.astype(BF16)
            p_low = (p_one - p_high.astype(F32)).astype(BF16)
            numer = lax.dot_general(probs.astype(BF16), vals, tn, preferred_element_type=F32)
            numer = numer + lax.dot_general(p_high, v_one, tn, preferred_element_type=F32)
            numer = numer + lax.dot_general(p_low, v_one, tn, preferred_element_type=F32)
            denom_col = jnp.transpose(jnp.broadcast_to(denom, (wide, wide)))[:, 0:1]
            result = (numer / denom_col).astype(BF16)
            for j in range(group):
                n = kv * group + j
                gath[0, rows, n * head:(n + 1) * head] = result[j * rg:(j + 1) * rg]
        return carry

    lax.fori_loop(0, n_groups, attend_group, 0)
    for h in range(2):
        for n in range(3):
            own_send(n, h, 1).start()
    for copy in locals_:
        copy.wait()

    def block_rows(place, j):
        off = place + (place // 2) * (5 - 2 * place)
        who = core + j * (1 - 2 * core)
        return (lax.rem(xi + off, nx) * 2 + who) * rb

    def y1(i):
        return pltpu.make_async_remote_copy(
            src_ref=pb.at[i, pl.ds(pl.multiple_of((1 - b1) * hb, hb), hb), :], dst_ref=r1.at[i],
            send_sem=y1s.at[i], recv_sem=y1r.at[i], **to_y(p1))

    def y2(i):
        return pltpu.make_async_remote_copy(
            src_ref=mq.at[i], dst_ref=r2.at[i], send_sem=y2s.at[i], recv_sem=y2r.at[i], **to_y(p2))

    def y3(i, base, mine):
        quarter = b2 if mine else 1 - b2
        rows = out_ref.at[pl.ds(pl.multiple_of(base + b1 * hb + quarter * qtr, qtr), qtr), :]
        return pltpu.make_async_remote_copy(
            src_ref=rows, dst_ref=rows, send_sem=y3s.at[i], recv_sem=y3r.at[i], **to_y(p2))

    def y4(i, base, mine):
        half = b1 if mine else 1 - b1
        rows = out_ref.at[pl.ds(pl.multiple_of(base + half * hb, hb), hb), :]
        return pltpu.make_async_remote_copy(
            src_ref=rows, dst_ref=rows, send_sem=y4s.at[i], recv_sem=y4r.at[i], **to_y(p1))

    for place in range(nx):
        if place == 1:
            for kind in range(2):
                for slot in (2, 4):
                    for h in range(2):
                        landed(slot, h, kind).wait_recv()
                for n in range(2):
                    opp_send(n, kind).start()
                for slot in (2, 4):
                    for h in range(2):
                        par_send(slot, h, kind).start()
        if place == 3:
            for kind in range(2):
                for h in range(2):
                    landed(6, h, kind).wait_recv()
                    par_send(6, h, kind).start()

        def product(j, carry, place=place):
            i = 2 * place + j

            @pl.when(j == 1)
            def _():
                for kind in range(2):
                    for h in range(2):
                        landed(2 * place + 1, h, kind).wait_recv()

            part = jnp.dot(gath[i], w2[...], preferred_element_type=F32)
            pb[i] = part.astype(BF16)
            mf[j] = part
            y1(i).start()
            return carry

        lax.fori_loop(0, 2, product, 0)
        for j in range(2):
            i = 2 * place + j
            y1(i).wait_recv()
            send_rows = pl.ds(pl.multiple_of(b1 * hb + (1 - b2) * qtr, qtr), qtr)
            send_sub = pl.ds(pl.multiple_of((1 - b2) * qtr, qtr), qtr)
            mq[i] = (mf[j, send_rows, :] + r1[i, send_sub, :].astype(F32)).astype(BF16)
            y2(i).start()
        for j in range(2):
            i = 2 * place + j
            y2(i).wait_recv()
            base = block_rows(place, j)
            keep_rows = pl.ds(pl.multiple_of(b1 * hb + b2 * qtr, qtr), qtr)
            keep_sub = pl.ds(pl.multiple_of(b2 * qtr, qtr), qtr)
            total = mf[j, keep_rows, :] + r1[i, keep_sub, :].astype(F32) + r2[i].astype(F32)
            rows = pl.ds(pl.multiple_of(base + b1 * hb + b2 * qtr, qtr), qtr)
            out_ref[rows, :] = (x_ref[rows, :].astype(F32) + total).astype(BF16)
            y3(i, base, True).start()
        for j in range(2):
            i = 2 * place + j
            base = block_rows(place, j)
            y3(i, base, False).wait_recv()
            y4(i, base, True).start()

    for place in range(nx):
        for j in range(2):
            i = 2 * place + j
            base = block_rows(place, j)
            y4(i, base, False).wait_recv()
            y1(i).wait_send()
            y2(i).wait_send()
            y3(i, base, True).wait_send()
            y4(i, base, True).wait_send()
    for kind in range(2):
        for h in range(2):
            for n in range(3):
                own_send(n, h, kind).wait_send()
            for slot in (2, 4, 6):
                par_send(slot, h, kind).wait_send()
        for n in range(2):
            opp_send(n, kind).wait_send()


def finish(nx, ny, act, qk, v_rows, k_cache, v_cache, positions, cos_a, sin_a, gains, gains_swap, w_out, w_down, x_in):
    rb, nf = act.shape
    kv_heads, ctx, head = k_cache.shape[1:]
    natt, wcols = w_out.shape
    heads = natt // head
    group = heads // kv_heads
    rg = 128 // group
    wide = group * rg
    col = jnp.arange(wide) % rg
    high = (positions.reshape(rb // rg, rg)[:, col] + ctx * col[None, :]).astype(jnp.int32)[:, None, :]
    vmem = pl.BlockSpec(memory_space=pltpu.VMEM)
    hbm = pl.BlockSpec(memory_space=ANY)
    dma = pltpu.SemaphoreType.DMA
    return pl.pallas_call(
        functools.partial(finish_kernel, nx, ny, heads, kv_heads),
        out_shape=(jax.ShapeDtypeStruct(x_in.shape, BF16), jax.ShapeDtypeStruct((kv_heads, rb, head), BF16)),
        in_specs=[hbm, vmem, vmem, hbm, hbm, vmem, vmem, vmem, vmem, vmem, hbm, hbm, vmem],
        out_specs=(vmem, vmem),
        scratch_shapes=[
            pltpu.VMEM((2 * nx, rb, natt + nf), BF16),
            pltpu.VMEM((natt + nf, wcols), BF16),
            pltpu.VMEM((heads + kv_heads, rb, head), BF16),
            pltpu.VMEM((2, rg, kv_heads, ctx, head), BF16),
            pltpu.VMEM((2, rg, kv_heads, ctx, head), BF16),
            pltpu.VMEM((2 * nx, rb, wcols), BF16),
            pltpu.VMEM((2 * nx, rb // 2, wcols), BF16),
            pltpu.VMEM((2, rb, wcols), F32),
            pltpu.VMEM((2 * nx, rb // 4, wcols), BF16),
            pltpu.VMEM((2 * nx, rb // 4, wcols), BF16),
            dma((3,)),
            dma((2, 2)),
            dma((3, 2, 2)),
            dma((2, 2)),
            dma((3, 2, 2)),
            dma((2 * nx, 2, 2)),
        ] + [dma((2 * nx,))] * 8,
        compiler_params=pltpu.CompilerParams(collective_id=1, has_side_effects=True, vmem_limit_bytes=VMEM_LIMIT),
        name='finish',
    )(act, qk, v_rows, k_cache, v_cache, high, cos_a, sin_a, gains, gains_swap, w_out, w_down, x_in)


def solution(mesh):
    dm_size = mesh.shape['dm']
    nx = dm_size // 2
    x_spec = P('dp', 'dm')
    row_spec = P(('dp', 'dm'))
    cache_spec = P(('dp', 'dm'), 'tp', None, None)
    new_spec = P(('dp', 'dm'), 'tp', None)
    hid_tp = P('dm', 'tp')
    tp_hid = P('tp', 'dm')
    head_spec = P('tp', None)

    def device_step(x_in, positions, k_cache, v_cache, ln_gain, w_q, w_k, w_v, w_gate, w_up, q_gain, k_gain, w_out, w_down):
        rows_loc = k_cache.shape[0]
        kv_loc = k_cache.shape[1]
        head_dim = k_cache.shape[3]
        hid = x_in.shape[1]
        d_model = hid * dm_size
        x_f32 = x_in.astype(jnp.float32)
        loc_mean = jnp.mean(x_f32, axis=1)
        loc_cent = x_f32 - loc_mean[:, None]
        loc_m2 = jnp.sum(loc_cent * loc_cent, axis=1)
        stats = lax.all_gather(jnp.stack([loc_mean, loc_m2]), 'dm', axis=0)
        row_mean = jnp.mean(stats[:, 0], axis=0)
        diff = stats[:, 0] - row_mean[None]
        row_var = (jnp.sum(stats[:, 1], axis=0) + hid * jnp.sum(diff * diff, axis=0)) / d_model
        normed = ((x_f32 - row_mean[:, None]) * lax.rsqrt(row_var + NORM_EPS)[:, None] * ln_gain.astype(jnp.float32)).astype(jnp.bfloat16)
        qk, v_rows, act = project(nx, normed, w_q, w_k, w_v, w_gate, w_up)
        inv_freq = ROPE_THETA ** (-(jnp.arange(head_dim) // 2 * 2).astype(jnp.float32) / head_dim)
        angles = positions.astype(jnp.float32)[:, None] * inv_freq[None, :]
        odd = jnp.arange(head_dim) % 2
        sin_a = jnp.sin(angles) * (2 * odd - 1).astype(jnp.float32)[None, :]
        gains = jnp.concatenate([q_gain, k_gain], axis=0).astype(jnp.float32)
        gains_swap = gains.reshape(-1, head_dim // 2, 2)[:, :, ::-1].reshape(gains.shape)
        x_out, k_heads = finish(nx, mesh.shape['tp'], act, qk, v_rows, k_cache, v_cache, positions, jnp.cos(angles), sin_a,
                                gains, gains_swap, w_out, w_down, x_in)
        k_new = jnp.transpose(k_heads, (1, 0, 2))
        v_new = v_rows.reshape(rows_loc, kv_loc, head_dim)
        return x_out, k_new, v_new

    return jax.shard_map(
        device_step,
        mesh=mesh,
        in_specs=(x_spec, row_spec, cache_spec, cache_spec, P('dm'), hid_tp, hid_tp, hid_tp, hid_tp, hid_tp, head_spec, head_spec, tp_hid, tp_hid),
        out_specs=(x_spec, new_spec, new_spec),
        check_vma=False,
    )
```

```python
import functools
import math

import jax
import jax.numpy as jnp
from jax import lax
from jax.experimental import pallas as pl
from jax.experimental.pallas import tpu as pltpu
from jax.sharding import PartitionSpec as P

NORM_EPS = 1e-5
ROPE_THETA = 75000000.0
MESH = pl.DeviceIdType.MESH
BF16 = jnp.bfloat16
F32 = jnp.float32
ANY = pl.ANY
VMEM_LIMIT = 66 * 1024 * 1000 - 1024 * 600


def project_kernel(nx, ntile, x_ref, gain_ref, wq_ref, wk_ref, wv_ref, wg_ref, wu_ref,
                   qkv_out, act_out,
                   xbuf, gain, stat, bq, bkv, bg, bu, rq, rkv, rg, lq, lkv, lu,
                   x_loc, x_snd, x_rcv, t_snd, t_rcv, w_loc, w_snd, w_rcv, r_snd, r_rcv):
    dm = lax.axis_index('dm')
    xi = dm // 2
    core = lax.rem(dm, 2)
    other = 2 * xi + 1 - core
    right = lax.rem(xi + 1, nx) * 2 + core
    left = lax.rem(xi + nx - 1, nx) * 2 + core
    rb = xbuf.shape[1]
    hb = rb // 2
    hid = x_ref.shape[1]
    tw = wg_ref.shape[1] // ntile

    every = slice(None)
    kw = wk_ref.shape[0]
    pieces = [(wq_ref, bq, 0, every), (wk_ref, bkv, 1, pl.ds(0, kw)), (wv_ref, bkv, 1, pl.ds(kw, kw))]
    for t in range(ntile):
        pieces.append((wg_ref, bg, 0, pl.ds(t * tw, tw)))
        pieces.append((wu_ref, bu, 0, pl.ds(t * tw, tw)))

    def x_local(j):
        return pltpu.make_async_copy(
            x_ref.at[pl.ds((2 * j + core) * rb, rb), :], xbuf.at[j, :, pl.ds(0, hid)], x_loc.at[j])

    def x_remote(j):
        return pltpu.make_async_remote_copy(
            src_ref=x_ref.at[pl.ds((2 * j + 1 - core) * rb, rb), :], dst_ref=xbuf.at[j, :, pl.ds(hid, hid)],
            send_sem=x_snd.at[j], recv_sem=x_rcv.at[j], device_id={'dm': other}, device_id_type=MESH)

    def w_place(n, start):
        _, dst, side, cut = pieces[n]
        return dst.at[cut, pl.ds(start, hid)] if side else dst.at[pl.ds(start, hid), cut]

    def w_source(n):
        src, _, side, cut = pieces[n]
        return src if side else src.at[:, cut]

    def w_local(n):
        return pltpu.make_async_copy(w_source(n), w_place(n, 0), w_loc.at[n])

    def w_remote(n):
        return pltpu.make_async_remote_copy(
            src_ref=w_source(n), dst_ref=w_place(n, hid), send_sem=w_snd.at[n], recv_sem=w_rcv.at[n],
            device_id={'dm': other}, device_id_type=MESH)

    def g_remote():
        return pltpu.make_async_remote_copy(
            src_ref=gain.at[:, pl.ds(0, hid)], dst_ref=gain.at[:, pl.ds(hid, hid)], send_sem=x_snd.at[nx], recv_sem=x_rcv.at[nx],
            device_id={'dm': other}, device_id_type=MESH)

    def t_remote(d):
        return pltpu.make_async_remote_copy(
            src_ref=stat.at[0], dst_ref=stat.at[d], send_sem=t_snd.at[d - 1], recv_sem=t_rcv.at[d - 1],
            device_id={'dm': lax.rem(xi + d, nx) * 2 + core}, device_id_type=MESH)

    gain[:, 0:hid] = jnp.broadcast_to(gain_ref[...].astype(F32), (8, hid))
    for j in range(nx):
        x_local(j).start()
    for n in range(len(pieces)):
        w_local(n).start()

    barrier = pltpu.get_barrier_semaphore()
    pl.semaphore_signal(barrier, inc=1, device_id={'dm': other}, device_id_type=MESH)
    for d in range(1, nx):
        pl.semaphore_signal(barrier, inc=1, device_id={'dm': lax.rem(xi + d, nx) * 2 + core}, device_id_type=MESH)
    pl.semaphore_wait(barrier, nx)

    for j in range(nx):
        x_remote(j).start()
    g_remote().start()
    for n in range(3):
        w_remote(n).start()

    for ref in (rq, rkv, rg, lq, lkv, lu):
        ref[0] = jnp.zeros(ref.shape[1:], ref.dtype)

    lane = lax.broadcasted_iota(jnp.int32, (rb, 128), 1)
    both = jnp.zeros((rb, 128), F32)
    for j in range(nx):
        x_local(j).wait()
        x_remote(j).wait()
        values = xbuf[j].astype(F32)
        mean = jnp.mean(values, axis=1, keepdims=True)
        centred = values - mean
        both = jnp.where(lane == 2 * j, mean, both)
        both = jnp.where(lane == 2 * j + 1, jnp.sum(centred * centred, axis=1, keepdims=True), both)
    for n in range(3, 5):
        w_remote(n).start()
    stat[0] = jnp.transpose(both)[:2 * nx]
    for d in range(1, nx):
        t_remote(d).start()
    g_remote().wait()
    for d in range(1, nx):
        t_remote(d).wait()
    parts = [stat[d] for d in range(nx)]
    total = sum(parts[1:], parts[0])
    row_mean = total / nx
    spread = sum([(p - row_mean) * (p - row_mean) for p in parts[1:]], (parts[0] - row_mean) * (parts[0] - row_mean))
    variance = (total + 2 * hid * pltpu.roll(spread, 1, 0)) / (2 * hid * nx)
    line = lax.broadcasted_iota(jnp.int32, total.shape, 0)
    both = jnp.where(lax.rem(line, 2) == 0, row_mean, lax.rsqrt(variance + NORM_EPS))
    both = jnp.transpose(jnp.concatenate([both, jnp.zeros((128 - 2 * nx, rb), F32)], axis=0))
    for j in range(nx):
        values = xbuf[j].astype(F32) - both[:, 2 * j:2 * j + 1]
        xbuf[j] = (values * both[:, 2 * j + 1:2 * j + 2] * gain[0:1, :]).astype(BF16)

    def hop(d, t, s, slot, cols):
        nxt = jnp.minimum(s + 1, nx - 1)
        return pltpu.make_async_remote_copy(
            src_ref=slot.at[s, :, cols], dst_ref=slot.at[nxt, :, cols],
            send_sem=r_snd.at[d, t, s], recv_sem=r_rcv.at[d, t, nxt],
            device_id={'dm': left if d else right}, device_id_type=MESH)

    def arrived(d, t, s, slot, cols):
        return pltpu.make_async_remote_copy(
            src_ref=slot.at[s, :, cols], dst_ref=slot.at[s, :, cols],
            send_sem=r_snd.at[d, t, s], recv_sem=r_rcv.at[d, t, s],
            device_id={'dm': left if d else right}, device_id_type=MESH)

    def partial(d, s, weight, w_cols):
        row = lax.rem(xi + 1 + s, nx) if d else lax.rem(xi + 2 * nx - 1 - s, nx)
        if w_cols is None:
            return lax.dot_general(xbuf[row, d * hb:(d + 1) * hb, :], weight[...], (((1,), (1,)), ((), ())),
                                   preferred_element_type=F32)
        return jnp.dot(xbuf[row], weight[:, w_cols], preferred_element_type=F32)

    def pass_on(part, d, t, s, slot, cols):
        @pl.when(s > 0)
        def _():
            arrived(d, t, s, slot, cols).wait_recv()

        slot[s, :, cols] = (part + slot[s, :, cols].astype(F32)).astype(BF16)

        @pl.when(s < nx - 1)
        def _():
            hop(d, t, s, slot, cols).start()

    def wait_piece(n):
        w_local(n).wait()
        w_remote(n).wait()

    half = rq.shape[2]

    def step(s, carry):
        @pl.when(s == 0)
        def _():
            wait_piece(0)
            for n in range(5, len(pieces)):
                if (n - 3) // 2 == 1:
                    w_remote(n).start()

        pass_on(partial(0, s, bq, pl.ds(0, half)), 0, 0, s, rq, pl.ds(0, half))
        pass_on(partial(1, s, bq, pl.ds(half, half)), 1, 0, s, lq, pl.ds(0, half))

        @pl.when(s == 0)
        def _():
            wait_piece(1)
            wait_piece(2)

        pass_on(partial(0, s, bkv, None), 0, 1, s, rkv, pl.ds(0, 2 * kw))
        pass_on(partial(1, s, bkv, None), 1, 1, s, lkv, pl.ds(0, 2 * kw))

        def mlp(t, inner):
            for now in range(ntile):
                @pl.when((s == 0) & (t == now))
                def _():
                    wait_piece(3 + 2 * now)
                    wait_piece(4 + 2 * now)
                    if 5 + 2 * now + 2 < len(pieces):
                        w_remote(7 + 2 * now).start()
                        w_remote(8 + 2 * now).start()

            cols = pl.ds(pl.multiple_of(t * tw, 128), tw)
            part_g = partial(0, s, bg, cols)
            part_u = partial(1, s, bu, cols)
            pass_on(part_g, 0, 2 + t, s, rg, cols)
            pass_on(part_u, 1, 2 + t, s, lu, cols)

            @pl.when(s == nx - 1)
            def _():
                gate = rg[nx - 1, :, cols].astype(F32)
                up = lu[nx - 1, :, cols].astype(F32)
                act_out[:, cols] = (gate / (1.0 + jnp.exp(-gate)) * up).astype(BF16)

            return inner

        return lax.fori_loop(0, ntile, mlp, carry)

    lax.fori_loop(0, nx, step, 0)
    qkv_out[:, :half] = rq[nx - 1]
    qkv_out[:, half:2 * half] = lq[nx - 1]
    qkv_out[:hb, 2 * half:] = rkv[nx - 1]
    qkv_out[hb:, 2 * half:] = lkv[nx - 1]

    def sent(s, carry):
        hop(0, 0, s, rq, pl.ds(0, half)).wait_send()
        hop(1, 0, s, lq, pl.ds(0, half)).wait_send()
        hop(0, 1, s, rkv, pl.ds(0, 2 * kw)).wait_send()
        hop(1, 1, s, lkv, pl.ds(0, 2 * kw)).wait_send()
        for t in range(ntile):
            cols = pl.ds(t * tw, tw)
            hop(0, 2 + t, s, rg, cols).wait_send()
            hop(1, 2 + t, s, lu, cols).wait_send()
        return carry

    lax.fori_loop(0, nx - 1, sent, 0)


def project(nx, x_in, gain, w_q, w_k_t, w_v_t, w_gate, w_up):
    rows, hid = x_in.shape
    rb = rows // (2 * nx)
    nq, nk, nf = w_q.shape[1], w_k_t.shape[0], w_gate.shape[1]
    ntile = 3
    npiece = 3 + 2 * ntile
    vmem = pl.BlockSpec(memory_space=pltpu.VMEM)
    dma = pltpu.SemaphoreType.DMA
    return pl.pallas_call(
        functools.partial(project_kernel, nx, ntile),
        out_shape=(jax.ShapeDtypeStruct((rb, nq + 2 * nk), BF16), jax.ShapeDtypeStruct((rb, nf), BF16)),
        in_specs=[pl.BlockSpec(memory_space=ANY), vmem] + [pl.BlockSpec(memory_space=ANY)] * 5,
        out_specs=(vmem,) * 2,
        scratch_shapes=[
            pltpu.VMEM((nx, rb, 2 * hid), BF16),
            pltpu.VMEM((8, 2 * hid), F32),
            pltpu.VMEM((nx, 2 * nx, rb), F32),
            pltpu.VMEM((2 * hid, nq), BF16),
            pltpu.VMEM((2 * nk, 2 * hid), BF16),
            pltpu.VMEM((2 * hid, nf), BF16),
            pltpu.VMEM((2 * hid, nf), BF16),
            pltpu.VMEM((nx, rb, nq // 2), BF16),
            pltpu.VMEM((nx, rb // 2, 2 * nk), BF16),
            pltpu.VMEM((nx, rb, nf), BF16),
            pltpu.VMEM((nx, rb, nq // 2), BF16),
            pltpu.VMEM((nx, rb // 2, 2 * nk), BF16),
            pltpu.VMEM((nx, rb, nf), BF16),
            dma((nx,)),
            dma((nx + 1,)),
            dma((nx + 1,)),
            dma((nx - 1,)),
            dma((nx - 1,)),
            dma((npiece,)),
            dma((npiece,)),
            dma((npiece,)),
            dma((2, 2 + ntile, nx)),
            dma((2, 2 + ntile, nx)),
        ],
        compiler_params=pltpu.CompilerParams(collective_id=0, has_side_effects=True, vmem_limit_bytes=VMEM_LIMIT),
        name='project',
    )(x_in, gain, w_q, w_k_t, w_v_t, w_gate, w_up)


def swap_pairs(v):
    length = v.shape[0]
    line = lax.broadcasted_iota(jnp.int32, v.shape, 0)
    return jnp.where(lax.rem(line, 2) == 0, pltpu.roll(v, length - 1, 0), pltpu.roll(v, 1, 0))


def finish_kernel(nx, ny, heads, kv_heads, act_ref, qkv_hbm, kc_ref, vc_ref, pos_ref, qgain_ref, kgain_ref,
                  wo_ref, wd_ref, x_hbm, out_ref, k_out, v_out,
                  qkv_ref, x_ref, gbuf, gath, w2, qt, kt, vt, sc, oc, ot, kbuf, vbuf, pb, r1, mf, mq, r2,
                  c_loc, kv_loc, s_own, s_opp, s_par, recv, y1s, y1r, y2s, y2r, y3s, y3r, y4s, y4r):
    dm = lax.axis_index('dm')
    y = lax.axis_index('tp')
    xi = dm // 2
    core = lax.rem(dm, 2)
    other = 2 * xi + 1 - core
    right = lax.rem(xi + 1, nx) * 2 + core
    left = lax.rem(xi + nx - 1, nx) * 2 + core
    nf = act_ref.shape[1]
    rb = act_ref.shape[0]
    hb, qtr = rb // 2, rb // 4
    head = qgain_ref.shape[1]
    natt = heads * head
    group = heads // kv_heads
    flip, mirror = y + 1 - 2 * lax.rem(y, 2), ny - 1 - y
    p1 = flip + core * (mirror - flip)
    p2 = mirror + core * (flip - mirror)
    bit_a, bit_b, bit_c = lax.rem((y + 1) // 2, 2), y // 2, lax.rem(y, 2)
    b1 = bit_a + core * (bit_b - bit_a)
    b2 = bit_b + core * (bit_c - bit_b)

    act_cols, att_cols = pl.ds(natt, nf), pl.ds(0, natt)

    def to(peer):
        return dict(device_id={'dm': peer}, device_id_type=MESH)

    def to_y(peer):
        return dict(device_id={'tp': peer}, device_id_type=MESH)

    def own_send(n, h, kind):
        peer, slot = ((right, 4), (left, 2), (other, 1))[n]
        cols = att_cols if kind else act_cols
        src = gath.at[0, pl.ds(h * hb, hb), cols] if kind else act_ref.at[pl.ds(h * hb, hb), :]
        return pltpu.make_async_remote_copy(
            src_ref=src, dst_ref=gath.at[slot, pl.ds(h * hb, hb), cols],
            send_sem=s_own.at[n, h, kind], recv_sem=recv.at[slot, h, kind], **to(peer))

    def opp_send(n, h, kind):
        peer, slot, sem = ((right, 4, 6), (left, 2, 2 * nx))[n]
        cols = att_cols if kind else act_cols
        rows = pl.ds(h * hb + n * qtr, qtr)
        return pltpu.make_async_remote_copy(
            src_ref=gath.at[slot, rows, cols], dst_ref=gath.at[6, rows, cols],
            send_sem=s_opp.at[n, h, kind], recv_sem=recv.at[sem, h, kind], **to(peer))

    def opp_landed(n, h, kind):
        cols = att_cols if kind else act_cols
        part = gath.at[6, pl.ds(h * hb + n * qtr, qtr), cols]
        return pltpu.make_async_remote_copy(
            src_ref=part, dst_ref=part, send_sem=s_opp.at[n, h, kind], recv_sem=recv.at[(6, 2 * nx)[n], h, kind], **to(other))

    def par_send(slot, h, kind):
        cols = att_cols if kind else act_cols
        return pltpu.make_async_remote_copy(
            src_ref=gath.at[slot, pl.ds(h * hb, hb), cols], dst_ref=gath.at[slot + 1, pl.ds(h * hb, hb), cols],
            send_sem=s_par.at[slot // 2 - 1, h, kind], recv_sem=recv.at[slot + 1, h, kind], **to(other))

    def landed(slot, h, kind):
        cols = att_cols if kind else act_cols
        part = gath.at[slot, pl.ds(h * hb, hb), cols]
        return pltpu.make_async_remote_copy(
            src_ref=part, dst_ref=part, send_sem=s_own.at[0, 0, 0], recv_sem=recv.at[slot, h, kind], **to(other))

    locals_ = [pltpu.make_async_copy(act_ref, gath.at[0, :, act_cols], c_loc.at[0]),
               pltpu.make_async_copy(wo_ref, w2.at[att_cols, :], c_loc.at[1]),
               pltpu.make_async_copy(wd_ref, w2.at[act_cols, :], c_loc.at[2]),
               pltpu.make_async_copy(x_hbm, x_ref, c_loc.at[3])]
    qkv_copy = pltpu.make_async_copy(qkv_hbm, qkv_ref, c_loc.at[4])
    qkv_copy.start()

    ctx = kc_ref.shape[1]
    cs = kbuf.shape[1]
    n_chunks = ctx // cs

    def cache_copy(side, idx):
        ref, buf = ((kc_ref, kbuf), (vc_ref, vbuf))[side]
        slot = lax.rem(idx, 2)
        return pltpu.make_async_copy(ref.at[idx // n_chunks, pl.ds(lax.rem(idx, n_chunks) * cs, cs)], buf.at[slot],
                                     kv_loc.at[side, slot])

    for side in range(2):
        cache_copy(side, 0).start()

    barrier = pltpu.get_barrier_semaphore()
    for peer in (other, right, left):
        pl.semaphore_signal(barrier, inc=1, **to(peer))
    for peer in (p1, p2):
        pl.semaphore_signal(barrier, inc=1, **to_y(peer))
    pl.semaphore_wait(barrier, 5)

    for h in range(2):
        for n in range(3):
            own_send(n, h, 0).start()
    for copy in locals_:
        copy.start()

    kv_wide = kv_heads * head
    gbuf[...] = jnp.zeros(gbuf.shape, F32)
    gbuf[0:heads, 0:head] = qgain_ref[...].astype(F32)
    gbuf[heads:heads + kv_heads, 0:head] = kgain_ref[...].astype(F32)
    gain_t = jnp.transpose(gbuf[...])
    gswap_t = swap_pairs(gain_t)
    line = lax.broadcasted_iota(jnp.int32, (head, rb), 0)
    odd = lax.rem(line, 2)
    inv_freq = jnp.exp((line - odd).astype(F32) * (-math.log(ROPE_THETA) / head))
    angles = inv_freq * pos_ref[...].astype(F32)
    cos_a = jnp.cos(angles)
    sin_a = jnp.sin(angles) * (2 * odd - 1).astype(F32)
    qkv_copy.wait()
    qkv_t = jnp.transpose(qkv_ref[...].astype(F32))
    swap_t = swap_pairs(qkv_t[:natt + kv_wide])
    for n in range(heads + kv_heads):
        own = slice(n * head, (n + 1) * head)
        one, two = qkv_t[own], swap_t[own]
        mean = jnp.mean(one, axis=0, keepdims=True)
        centred = one - mean
        scale = lax.rsqrt(jnp.mean(centred * centred, axis=0, keepdims=True) + NORM_EPS)
        turned = (centred * scale * gain_t[:head, n:n + 1] * cos_a
                  + (two - mean) * scale * gswap_t[:head, n:n + 1] * sin_a)
        turned = turned.astype(BF16)
        if n < heads:
            qt[n] = turned.astype(F32)
        else:
            k_out[n - heads] = turned
            kt[n - heads] = turned.astype(F32)
    for n in range(kv_heads):
        one = qkv_t[natt + kv_wide + n * head:natt + kv_wide + (n + 1) * head]
        vt[n] = one
        v_out[n] = one.astype(BF16)

    score_scale = head ** -0.5
    db = 16

    def attend_head(kv, carry):
        first = kv * group

        def score_chunk(c, inner):
            idx = kv * n_chunks + c
            slot = lax.rem(idx, 2)
            cache_copy(0, idx).wait()

            @pl.when(idx < kv_heads * n_chunks - 1)
            def _():
                cache_copy(0, idx + 1).start()

            def score(s, deep):
                keys = kbuf[slot, s].astype(F32)
                sc[c * cs + s] = jnp.concatenate(
                    [jnp.sum(qt[first + j] * keys, axis=0, keepdims=True) for j in range(group)], axis=0)
                return deep

            return lax.fori_loop(0, cs, score, inner)

        lax.fori_loop(0, n_chunks, score_chunk, 0)
        k_one = kt[kv]
        s_one = jnp.concatenate([jnp.sum(qt[first + j] * k_one, axis=0, keepdims=True) for j in range(group)], axis=0) * score_scale
        scores = sc[...] * score_scale
        at = lax.broadcasted_iota(jnp.int32, scores.shape, 0)
        scores = jnp.where(at < pos_ref[...][None], scores, -1e30)
        top = jnp.maximum(jnp.max(scores, axis=0), s_one)
        probs = jnp.exp(scores - top[None])
        p_one = jnp.exp(s_one - top)
        denom = jnp.sum(probs, axis=0) + p_one
        sc[...] = probs.astype(BF16).astype(F32)
        v_one = vt[kv]
        for j in range(group):
            oc[j] = p_one[j:j + 1] * v_one

        def value_chunk(c, inner):
            idx = kv * n_chunks + c
            slot = lax.rem(idx, 2)
            cache_copy(1, idx).wait()

            @pl.when(idx < kv_heads * n_chunks - 1)
            def _():
                cache_copy(1, idx + 1).start()

            def value(b, deep):
                lines = pl.ds(pl.multiple_of(b * db, db), db)
                sums = [oc[j, lines, :] for j in range(group)]
                for s in range(cs):
                    vals = vbuf[slot, s, lines, :].astype(F32)
                    for j in range(group):
                        sums[j] = sums[j] + sc[c * cs + s, j:j + 1, :] * vals
                for j in range(group):
                    oc[j, lines, :] = sums[j]
                return deep

            return lax.fori_loop(0, head // db, value, inner)

        lax.fori_loop(0, n_chunks, value_chunk, 0)
        for j in range(group):
            lines = pl.ds(pl.multiple_of((first + j) * head, 8), head)
            ot[lines, :] = oc[j] / denom[j:j + 1]
        return carry

    lax.fori_loop(0, kv_heads, attend_head, 0)
    gath[0, :, 0:natt] = jnp.transpose(ot[...]).astype(BF16)
    for h in range(2):
        for n in range(3):
            own_send(n, h, 1).start()
    for copy in locals_:
        copy.wait()

    def block_rows(place, j):
        off = place + (place // 2) * (5 - 2 * place)
        who = core + j * (1 - 2 * core)
        return (lax.rem(xi + off, nx) * 2 + who) * rb

    groups = [(place, 0, rb) for place in range(nx - 1)] + [(nx - 1, 0, hb), (nx - 1, hb, hb)]

    def aligned(start, size):
        return pl.ds(pl.multiple_of(start, size), size)

    def y1(g, j):
        place, row0, size = groups[g]
        i = 2 * place + j
        return pltpu.make_async_remote_copy(
            src_ref=pb.at[i, aligned(row0 + (1 - b1) * (size // 2), size // 2), :], dst_ref=r1.at[i, pl.ds(row0 // 2, size // 2), :],
            send_sem=y1s.at[2 * g + j], recv_sem=y1r.at[2 * g + j], **to_y(p1))

    def y2(g, j):
        place, row0, size = groups[g]
        i = 2 * place + j
        rows = pl.ds(row0 // 4, size // 4)
        return pltpu.make_async_remote_copy(
            src_ref=mq.at[i, rows, :], dst_ref=r2.at[i, rows, :],
            send_sem=y2s.at[2 * g + j], recv_sem=y2r.at[2 * g + j], **to_y(p2))

    def y3(g, j, mine):
        place, row0, size = groups[g]
        quarter = b2 if mine else 1 - b2
        start = block_rows(place, j) + row0 + b1 * (size // 2) + quarter * (size // 4)
        rows = out_ref.at[aligned(start, size // 4), :]
        return pltpu.make_async_remote_copy(
            src_ref=rows, dst_ref=rows, send_sem=y3s.at[2 * g + j], recv_sem=y3r.at[2 * g + j], **to_y(p2))

    def y4(g, j, mine):
        place, row0, size = groups[g]
        half = b1 if mine else 1 - b1
        rows = out_ref.at[aligned(block_rows(place, j) + row0 + half * (size // 2), size // 2), :]
        return pltpu.make_async_remote_copy(
            src_ref=rows, dst_ref=rows, send_sem=y4s.at[2 * g + j], recv_sem=y4r.at[2 * g + j], **to_y(p1))

    def product(g, kinds=(0, 1)):
        place, row0, size = groups[g]
        rows = pl.ds(row0, size)
        if len(kinds) == 2:
            cols = slice(None)
        else:
            cols = att_cols if kinds[0] else act_cols

        def body(j, carry):
            i = 2 * place + j

            @pl.when(j == 1)
            def _():
                for kind in kinds:
                    for h in range(row0 // hb, (row0 + size) // hb):
                        landed(2 * place + 1, h, kind).wait_recv()

            part = jnp.dot(gath[i, rows, cols], w2[cols, :], preferred_element_type=F32)
            if kinds == (1,):
                part = part + mf[i, rows, :]
            mf[i, rows, :] = part
            if 1 in kinds:
                pb[i, rows, :] = part.astype(BF16)
                y1(g, j).start()
            return carry

        lax.fori_loop(0, 2, body, 0)

    def stage2(g):
        place, row0, size = groups[g]
        for j in range(2):
            i = 2 * place + j
            y1(g, j).wait_recv()
            rows = aligned(row0 + b1 * (size // 2) + (1 - b2) * (size // 4), size // 4)
            sub = aligned(row0 // 2 + (1 - b2) * (size // 4), size // 4)
            mq[i, row0 // 4:(row0 + size) // 4, :] = (mf[i, rows, :] + r1[i, sub, :].astype(F32)).astype(BF16)
            y2(g, j).start()

    def stage3(g):
        place, row0, size = groups[g]
        for j in range(2):
            i = 2 * place + j
            y2(g, j).wait_recv()
            rows = aligned(row0 + b1 * (size // 2) + b2 * (size // 4), size // 4)
            sub = aligned(row0 // 2 + b2 * (size // 4), size // 4)
            total = mf[i, rows, :] + r1[i, sub, :].astype(F32) + r2[i, row0 // 4:(row0 + size) // 4, :].astype(F32)
            rows = aligned(block_rows(place, j) + row0 + b1 * (size // 2) + b2 * (size // 4), size // 4)
            out_ref[rows, :] = (x_ref[rows, :].astype(F32) + total).astype(BF16)
            y3(g, j, True).start()

    def stage4(g):
        for j in range(2):
            y3(g, j, False).wait_recv()
            y4(g, j, True).start()

    def near_landed(kind):
        for slot in (2, 4):
            for h in range(2):
                landed(slot, h, kind).wait_recv()
        if kind == 0:
            forwards = ((0, 0),)
        else:
            forwards = ((0, 1), (1, 0), (1, 1))
        for h, k in forwards:
            for n in range(2):
                opp_send(n, h, k).start()
        for slot in (2, 4):
            for h in range(2):
                par_send(slot, h, kind).start()

    def far_landed(h, kind):
        for n in range(2):
            opp_landed(n, h, kind).wait_recv()
        par_send(6, h, kind).start()

    product(0)
    stage2(0)
    near_landed(0)
    stage3(0)
    near_landed(1)
    stage4(0)
    product(1)
    product(2)
    stage2(1)
    stage2(2)
    far_landed(0, 0)
    far_landed(0, 1)
    stage3(1)
    stage3(2)
    product(3)
    stage4(1)
    stage4(2)
    stage2(3)
    stage3(3)
    far_landed(1, 0)
    product(4, (0,))
    far_landed(1, 1)
    product(4, (1,))
    stage4(3)
    stage2(4)
    stage3(4)
    stage4(4)

    for g in range(len(groups)):
        for j in range(2):
            y4(g, j, False).wait_recv()
            y1(g, j).wait_send()
            y2(g, j).wait_send()
            y3(g, j, True).wait_send()
            y4(g, j, True).wait_send()
    for kind in range(2):
        for h in range(2):
            for n in range(3):
                own_send(n, h, kind).wait_send()
            for slot in (2, 4, 6):
                par_send(slot, h, kind).wait_send()
            for n in range(2):
                opp_send(n, h, kind).wait_send()


def finish(nx, ny, act, qkv, k_cache, v_cache, positions, q_gain, k_gain, w_out, w_down, x_in):
    rb, nf = act.shape
    kv_heads, ctx, head = k_cache.shape[:3]
    natt, wcols = w_out.shape
    heads = natt // head
    group = heads // kv_heads
    cs = 16
    vmem = pl.BlockSpec(memory_space=pltpu.VMEM)
    hbm = pl.BlockSpec(memory_space=ANY)
    dma = pltpu.SemaphoreType.DMA
    new = jax.ShapeDtypeStruct((kv_heads, head, rb), BF16)
    return pl.pallas_call(
        functools.partial(finish_kernel, nx, ny, heads, kv_heads),
        out_shape=(jax.ShapeDtypeStruct(x_in.shape, BF16), new, new),
        in_specs=[hbm, hbm, hbm, hbm, vmem, vmem, vmem, hbm, hbm, hbm],
        out_specs=(vmem, vmem, vmem),
        scratch_shapes=[
            pltpu.VMEM(qkv.shape, BF16),
            pltpu.VMEM(x_in.shape, BF16),
            pltpu.VMEM((128, pl.cdiv(head, 128) * 128), F32),
            pltpu.VMEM((2 * nx, rb, natt + nf), BF16),
            pltpu.VMEM((natt + nf, wcols), BF16),
            pltpu.VMEM((heads, head, rb), F32),
            pltpu.VMEM((kv_heads, head, rb), F32),
            pltpu.VMEM((kv_heads, head, rb), F32),
            pltpu.VMEM((ctx, group, rb), F32),
            pltpu.VMEM((group, head, rb), F32),
            pltpu.VMEM((natt, rb), F32),
            pltpu.VMEM((2, cs, head, rb), BF16),
            pltpu.VMEM((2, cs, head, rb), BF16),
            pltpu.VMEM((2 * nx, rb, wcols), BF16),
            pltpu.VMEM((2 * nx, rb // 2, wcols), BF16),
            pltpu.VMEM((2 * nx, rb, wcols), F32),
            pltpu.VMEM((2 * nx, rb // 4, wcols), BF16),
            pltpu.VMEM((2 * nx, rb // 4, wcols), BF16),
            dma((5,)),
            dma((2, 2)),
            dma((3, 2, 2)),
            dma((2, 2, 2)),
            dma((3, 2, 2)),
            dma((2 * nx + 1, 2, 2)),
        ] + [dma((2 * nx + 2,))] * 8,
        compiler_params=pltpu.CompilerParams(collective_id=1, has_side_effects=True, vmem_limit_bytes=VMEM_LIMIT),
        name='finish',
    )(act, qkv, k_cache, v_cache, positions, q_gain, k_gain, w_out, w_down, x_in)


def settle_kernel(n_parts, x_ref, k_ref, v_ref, x_out, k_out, v_out, xbuf, kbuf, vbuf, sem_in, sem_out):
    rows = x_ref.shape[0] // n_parts
    moves = [(x_ref.at[pl.ds(n * rows, rows)], xbuf.at[pl.ds(n * rows, rows)], x_out.at[pl.ds(n * rows, rows)]) for n in range(n_parts)]
    moves += [(k_ref, kbuf, k_out), (v_ref, vbuf, v_out)]
    for n, (src, mid, _) in enumerate(moves):
        pltpu.make_async_copy(src, mid, sem_in.at[n]).start()
    for n, (src, mid, dst) in enumerate(moves):
        pltpu.make_async_copy(src, mid, sem_in.at[n]).wait()
        pltpu.make_async_copy(mid, dst, sem_out.at[n]).start()
    for n, (_, mid, dst) in enumerate(moves):
        pltpu.make_async_copy(mid, dst, sem_out.at[n]).wait()


def settle(x_out, k_t, v_t):
    n_parts = 4
    hbm = pl.BlockSpec(memory_space=ANY)
    arrays = (x_out, k_t, v_t)
    return pl.pallas_call(
        functools.partial(settle_kernel, n_parts),
        out_shape=tuple(jax.ShapeDtypeStruct(a.shape, a.dtype) for a in arrays),
        in_specs=[hbm] * 3,
        out_specs=(hbm,) * 3,
        scratch_shapes=[pltpu.VMEM(a.shape, a.dtype) for a in arrays] + [pltpu.SemaphoreType.DMA((n_parts + 2,))] * 2,
        name='settle',
    )(*arrays)


def solution(mesh):
    dm_size = mesh.shape['dm']
    nx = dm_size // 2
    x_spec = P('dp', 'dm')
    row_spec = P(('dp', 'dm'))
    cache_spec = P(('dp', 'dm'), 'tp', None, None)
    new_spec = P(('dp', 'dm'), 'tp', None)
    hid_tp = P('dm', 'tp')
    tp_hid = P('tp', 'dm')
    head_spec = P('tp', None)

    def device_step(x_in, positions, k_cache, v_cache, ln_gain, w_q, w_k, w_v, w_gate, w_up, q_gain, k_gain, w_out, w_down):
        qkv, act = project(nx, x_in, ln_gain[None, :], w_q, w_k.T, w_v.T, w_gate, w_up)
        x_out, k_t, v_t = settle(*finish(
            nx, mesh.shape['tp'], act, qkv, jnp.transpose(k_cache, (1, 2, 3, 0)), jnp.transpose(v_cache, (1, 2, 3, 0)),
            positions[None, :], q_gain, k_gain, w_out, w_down, x_in))
        k_new = jnp.transpose(k_t, (2, 0, 1))
        v_new = jnp.transpose(v_t, (2, 0, 1))
        return x_out, k_new, v_new

    return jax.shard_map(
        device_step,
        mesh=mesh,
        in_specs=(x_spec, row_spec, cache_spec, cache_spec, P('dm'), hid_tp, hid_tp, hid_tp, hid_tp, hid_tp, head_spec, head_spec, tp_hid, tp_hid),
        out_specs=(x_spec, new_spec, new_spec),
        check_vma=False,
    )
```

```python
import functools
import math

import jax
import jax.numpy as jnp
from jax import lax
from jax.experimental import pallas as pl
from jax.experimental.pallas import tpu as pltpu
from jax.sharding import PartitionSpec as P

NORM_EPS = 1e-5
ROPE_THETA = 75000000.0
MESH = pl.DeviceIdType.MESH
BF16 = jnp.bfloat16
F32 = jnp.float32
ANY = pl.ANY
VMEM_LIMIT = 66 * 1024 * 1000 - 1024 * 600


def project_kernel(nx, nload, ntile, x_ref, gain_ref, wq_ref, wk_ref, wv_ref, wg_ref, wu_ref,
                   qkv_out, act_out,
                   xbuf, gain, stat, bq, bkv, bg, bu, rq, rkv, rg, lq, lkv, lu, qkv_buf, act_buf,
                   o_sem, x_loc, x_snd, x_rcv, t_snd, t_rcv, w_loc, w_snd, w_rcv, r_snd, r_rcv):
    dm = lax.axis_index('dm')
    xi = dm // 2
    core = lax.rem(dm, 2)
    other = 2 * xi + 1 - core
    right = lax.rem(xi + 1, nx) * 2 + core
    left = lax.rem(xi + nx - 1, nx) * 2 + core
    rb = xbuf.shape[1]
    hb = rb // 2
    hid = x_ref.shape[1]
    tw = wg_ref.shape[1] // ntile
    lw = wg_ref.shape[1] // nload
    per = ntile // nload

    every = slice(None)
    kw = wk_ref.shape[0]
    pieces = [(wq_ref, bq, 0, every), (wk_ref, bkv, 1, pl.ds(0, kw)), (wv_ref, bkv, 1, pl.ds(kw, kw))]
    for n in range(nload):
        pieces.append((wg_ref, bg, 0, pl.ds(n * lw, lw)))
        pieces.append((wu_ref, bu, 0, pl.ds(n * lw, lw)))

    def x_local(j):
        return pltpu.make_async_copy(
            x_ref.at[pl.ds((2 * j + core) * rb, rb), :], xbuf.at[j, :, pl.ds(0, hid)], x_loc.at[j])

    def x_remote(j):
        return pltpu.make_async_remote_copy(
            src_ref=x_ref.at[pl.ds((2 * j + 1 - core) * rb, rb), :], dst_ref=xbuf.at[j, :, pl.ds(hid, hid)],
            send_sem=x_snd.at[j], recv_sem=x_rcv.at[j], device_id={'dm': other}, device_id_type=MESH)

    def w_place(n, start):
        _, dst, side, cut = pieces[n]
        return dst.at[cut, pl.ds(start, hid)] if side else dst.at[pl.ds(start, hid), cut]

    def w_source(n):
        src, _, side, cut = pieces[n]
        return src if side else src.at[:, cut]

    def w_local(n):
        return pltpu.make_async_copy(w_source(n), w_place(n, 0), w_loc.at[n])

    def w_remote(n):
        return pltpu.make_async_remote_copy(
            src_ref=w_source(n), dst_ref=w_place(n, hid), send_sem=w_snd.at[n], recv_sem=w_rcv.at[n],
            device_id={'dm': other}, device_id_type=MESH)

    def g_remote():
        return pltpu.make_async_remote_copy(
            src_ref=gain.at[:, pl.ds(0, hid)], dst_ref=gain.at[:, pl.ds(hid, hid)], send_sem=x_snd.at[nx], recv_sem=x_rcv.at[nx],
            device_id={'dm': other}, device_id_type=MESH)

    def t_remote(d):
        return pltpu.make_async_remote_copy(
            src_ref=stat.at[0], dst_ref=stat.at[d], send_sem=t_snd.at[d - 1], recv_sem=t_rcv.at[d - 1],
            device_id={'dm': lax.rem(xi + d, nx) * 2 + core}, device_id_type=MESH)

    gain[:, 0:hid] = jnp.broadcast_to(gain_ref[...].astype(F32)[None, :], (8, hid))
    for j in range(nx):
        x_local(j).start()
    for n in range(len(pieces)):
        w_local(n).start()

    barrier = pltpu.get_barrier_semaphore()
    pl.semaphore_signal(barrier, inc=1, device_id={'dm': other}, device_id_type=MESH)
    for d in range(1, nx):
        pl.semaphore_signal(barrier, inc=1, device_id={'dm': lax.rem(xi + d, nx) * 2 + core}, device_id_type=MESH)
    pl.semaphore_wait(barrier, nx)

    for j in range(nx):
        x_remote(j).start()
    g_remote().start()
    w_remote(0).start()

    for ref in (rq, rkv, rg, lq, lkv, lu):
        ref[0] = jnp.zeros(ref.shape[1:], ref.dtype)

    lane = lax.broadcasted_iota(jnp.int32, (rb, 128), 1)
    both = jnp.zeros((rb, 128), F32)
    for j in range(nx):
        x_local(j).wait()
        x_remote(j).wait()
        values = xbuf[j].astype(F32)
        mean = jnp.mean(values, axis=1, keepdims=True)
        centred = values - mean
        both = jnp.where(lane == 2 * j, mean, both)
        both = jnp.where(lane == 2 * j + 1, jnp.sum(centred * centred, axis=1, keepdims=True), both)
    for n in range(1, 5):
        w_remote(n).start()
    stat[0] = jnp.transpose(both)[:2 * nx]
    for d in range(1, nx):
        t_remote(d).start()
    g_remote().wait()
    for d in range(1, nx):
        t_remote(d).wait()
    parts = [stat[d] for d in range(nx)]
    total = sum(parts[1:], parts[0])
    row_mean = total / nx
    spread = sum([(p - row_mean) * (p - row_mean) for p in parts[1:]], (parts[0] - row_mean) * (parts[0] - row_mean))
    variance = (total + 2 * hid * pltpu.roll(spread, 1, 0)) / (2 * hid * nx)
    line = lax.broadcasted_iota(jnp.int32, total.shape, 0)
    both = jnp.where(lax.rem(line, 2) == 0, row_mean, lax.rsqrt(variance + NORM_EPS))
    both = jnp.transpose(jnp.concatenate([both, jnp.zeros((128 - 2 * nx, rb), F32)], axis=0))
    for j in range(nx):
        values = xbuf[j].astype(F32) - both[:, 2 * j:2 * j + 1]
        xbuf[j] = (values * both[:, 2 * j + 1:2 * j + 2] * gain[0:1, :]).astype(BF16)

    def hop(d, t, s, slot, cols):
        nxt = jnp.minimum(s + 1, nx - 1)
        return pltpu.make_async_remote_copy(
            src_ref=slot.at[s, :, cols], dst_ref=slot.at[nxt, :, cols],
            send_sem=r_snd.at[d, t, s], recv_sem=r_rcv.at[d, t, nxt],
            device_id={'dm': left if d else right}, device_id_type=MESH)

    def arrived(d, t, s, slot, cols):
        return pltpu.make_async_remote_copy(
            src_ref=slot.at[s, :, cols], dst_ref=slot.at[s, :, cols],
            send_sem=r_snd.at[d, t, s], recv_sem=r_rcv.at[d, t, s],
            device_id={'dm': left if d else right}, device_id_type=MESH)

    def partial(d, s, weight, w_cols):
        row = lax.rem(xi + 1 + s, nx) if d else lax.rem(xi + 2 * nx - 1 - s, nx)
        if w_cols is None:
            return lax.dot_general(xbuf[row, d * hb:(d + 1) * hb, :], weight[...], (((1,), (1,)), ((), ())),
                                   preferred_element_type=F32)
        return jnp.dot(xbuf[row], weight[:, w_cols], preferred_element_type=F32)

    def pass_on(part, d, t, s, slot, cols):
        @pl.when(s > 0)
        def _():
            arrived(d, t, s, slot, cols).wait_recv()

        slot[s, :, cols] = (part + slot[s, :, cols].astype(F32)).astype(BF16)

        @pl.when(s < nx - 1)
        def _():
            hop(d, t, s, slot, cols).start()

    def wait_piece(n):
        w_local(n).wait()
        w_remote(n).wait()

    half = rq.shape[2]
    qkv_leave = pltpu.make_async_copy(qkv_buf, qkv_out, o_sem.at[ntile])

    def act_leave(t):
        cols = pl.ds(pl.multiple_of(t * tw, 128), tw)
        return pltpu.make_async_copy(act_buf.at[:, cols], act_out.at[:, cols], o_sem.at[t])


    def step(s, carry):
        @pl.when(s == 0)
        def _():
            wait_piece(0)
            for n in range(5, len(pieces)):
                if (n - 3) // 2 == 1:
                    w_remote(n).start()

        pass_on(partial(0, s, bq, pl.ds(0, half)), 0, 0, s, rq, pl.ds(0, half))
        pass_on(partial(1, s, bq, pl.ds(half, half)), 1, 0, s, lq, pl.ds(0, half))

        @pl.when(s == 0)
        def _():
            wait_piece(1)
            wait_piece(2)

        pass_on(partial(0, s, bkv, None), 0, 1, s, rkv, pl.ds(0, 2 * kw))
        pass_on(partial(1, s, bkv, None), 1, 1, s, lkv, pl.ds(0, 2 * kw))

        @pl.when(s == nx - 1)
        def _():
            qkv_buf[:, :half] = rq[nx - 1]
            qkv_buf[:, half:2 * half] = lq[nx - 1]
            qkv_buf[:hb, 2 * half:] = rkv[nx - 1]
            qkv_buf[hb:, 2 * half:] = lkv[nx - 1]
            qkv_leave.start()

        def mlp(t, inner):
            for now in range(nload):
                @pl.when((s == 0) & (t == now * per))
                def _():
                    wait_piece(3 + 2 * now)
                    wait_piece(4 + 2 * now)
                    if 5 + 2 * now + 2 < len(pieces):
                        w_remote(7 + 2 * now).start()
                        w_remote(8 + 2 * now).start()

            cols = pl.ds(pl.multiple_of(t * tw, 128), tw)
            part_g = partial(0, s, bg, cols)
            part_u = partial(1, s, bu, cols)
            pass_on(part_g, 0, 2 + t, s, rg, cols)
            pass_on(part_u, 1, 2 + t, s, lu, cols)

            @pl.when(s == nx - 1)
            def _():
                gate = rg[nx - 1, :, cols].astype(F32)
                up = lu[nx - 1, :, cols].astype(F32)
                act_buf[:, cols] = (gate / (1.0 + jnp.exp(-gate)) * up).astype(BF16)
                act_leave(t).start()

            return inner

        return lax.fori_loop(0, ntile, mlp, carry)

    lax.fori_loop(0, nx, step, 0)
    def sent(s, carry):
        hop(0, 0, s, rq, pl.ds(0, half)).wait_send()
        hop(1, 0, s, lq, pl.ds(0, half)).wait_send()
        hop(0, 1, s, rkv, pl.ds(0, 2 * kw)).wait_send()
        hop(1, 1, s, lkv, pl.ds(0, 2 * kw)).wait_send()
        def sent_mlp(t, inner):
            cols = pl.ds(pl.multiple_of(t * tw, 128), tw)
            hop(0, 2 + t, s, rg, cols).wait_send()
            hop(1, 2 + t, s, lu, cols).wait_send()
            return inner

        return lax.fori_loop(0, ntile, sent_mlp, carry)

    lax.fori_loop(0, nx - 1, sent, 0)
    qkv_leave.wait()

    def left_all(t, carry):
        act_leave(t).wait()
        return carry

    lax.fori_loop(0, ntile, left_all, 0)


def project(nx, x_in, gain, w_q, w_k_t, w_v_t, w_gate, w_up):
    rows, hid = x_in.shape
    rb = rows // (2 * nx)
    nq, nk, nf = w_q.shape[1], w_k_t.shape[0], w_gate.shape[1]
    nload, ntile = 3, 9
    npiece = 3 + 2 * nload
    vmem = pl.BlockSpec(memory_space=pltpu.VMEM)
    dma = pltpu.SemaphoreType.DMA
    return pl.pallas_call(
        functools.partial(project_kernel, nx, nload, ntile),
        out_shape=(jax.ShapeDtypeStruct((rb, nq + 2 * nk), BF16), jax.ShapeDtypeStruct((rb, nf), BF16)),
        in_specs=[pl.BlockSpec(memory_space=ANY), vmem] + [pl.BlockSpec(memory_space=ANY)] * 5,
        out_specs=(pl.BlockSpec(memory_space=ANY),) * 2,
        scratch_shapes=[
            pltpu.VMEM((nx, rb, 2 * hid), BF16),
            pltpu.VMEM((8, 2 * hid), F32),
            pltpu.VMEM((nx, 2 * nx, rb), F32),
            pltpu.VMEM((2 * hid, nq), BF16),
            pltpu.VMEM((2 * nk, 2 * hid), BF16),
            pltpu.VMEM((2 * hid, nf), BF16),
            pltpu.VMEM((2 * hid, nf), BF16),
            pltpu.VMEM((nx, rb, nq // 2), BF16),
            pltpu.VMEM((nx, rb // 2, 2 * nk), BF16),
            pltpu.VMEM((nx, rb, nf), BF16),
            pltpu.VMEM((nx, rb, nq // 2), BF16),
            pltpu.VMEM((nx, rb // 2, 2 * nk), BF16),
            pltpu.VMEM((nx, rb, nf), BF16),
            pltpu.VMEM((rb, nq + 2 * nk), BF16),
            pltpu.VMEM((rb, nf), BF16),
            dma((ntile + 1,)),
            dma((nx,)),
            dma((nx + 1,)),
            dma((nx + 1,)),
            dma((nx - 1,)),
            dma((nx - 1,)),
            dma((npiece,)),
            dma((npiece,)),
            dma((npiece,)),
            dma((2, 2 + ntile, nx)),
            dma((2, 2 + ntile, nx)),
        ],
        compiler_params=pltpu.CompilerParams(collective_id=0, has_side_effects=True, vmem_limit_bytes=VMEM_LIMIT),
        name='project',
    )(x_in, gain, w_q, w_k_t, w_v_t, w_gate, w_up)


def swap_pairs(v):
    length = v.shape[0]
    line = lax.broadcasted_iota(jnp.int32, v.shape, 0)
    return jnp.where(lax.rem(line, 2) == 0, pltpu.roll(v, length - 1, 0), pltpu.roll(v, 1, 0))


def finish_kernel(nx, ny, heads, kv_heads, act_ref, qkv_hbm, kc_ref, vc_ref, pos_ref, qgain_ref, kgain_ref,
                  wo_ref, wd_ref, x_hbm, out_hbm, k_hbm, v_hbm,
                  out_ref, k_out, v_out, o_sem, qkv_ref, x_ref, gbuf, gath, w2, qt, kt, vt, sc, oc, ot, kbuf, vbuf, pb, r1, mf, mq, r2,
                  c_loc, kv_loc, s_own, s_opp, s_par, recv, y1s, y1r, y2s, y2r, y3s, y3r, y4s, y4r):
    dm = lax.axis_index('dm')
    y = lax.axis_index('tp')
    xi = dm // 2
    core = lax.rem(dm, 2)
    other = 2 * xi + 1 - core
    right = lax.rem(xi + 1, nx) * 2 + core
    left = lax.rem(xi + nx - 1, nx) * 2 + core
    nf = act_ref.shape[1]
    rb = act_ref.shape[0]
    hb, qtr = rb // 2, rb // 4
    head = qgain_ref.shape[1]
    natt = heads * head
    group = heads // kv_heads
    flip, mirror = y + 1 - 2 * lax.rem(y, 2), ny - 1 - y
    p1 = flip + core * (mirror - flip)
    p2 = mirror + core * (flip - mirror)
    bit_a, bit_b, bit_c = lax.rem((y + 1) // 2, 2), y // 2, lax.rem(y, 2)
    b1 = bit_a + core * (bit_b - bit_a)
    b2 = bit_b + core * (bit_c - bit_b)

    act_cols, att_cols = pl.ds(natt, nf), pl.ds(0, natt)

    def to(peer):
        return dict(device_id={'dm': peer}, device_id_type=MESH)

    def to_y(peer):
        return dict(device_id={'tp': peer}, device_id_type=MESH)

    def own_send(n, h, kind):
        peer, slot = ((right, 4), (left, 2), (other, 1))[n]
        cols = att_cols if kind else act_cols
        src = gath.at[0, pl.ds(h * hb, hb), cols] if kind else act_ref.at[pl.ds(h * hb, hb), :]
        return pltpu.make_async_remote_copy(
            src_ref=src, dst_ref=gath.at[slot, pl.ds(h * hb, hb), cols],
            send_sem=s_own.at[n, h, kind], recv_sem=recv.at[slot, h, kind], **to(peer))

    def opp_send(n, h, kind):
        peer, slot, sem = ((right, 4, 6), (left, 2, 2 * nx))[n]
        cols = att_cols if kind else act_cols
        rows = pl.ds(h * hb + n * qtr, qtr)
        return pltpu.make_async_remote_copy(
            src_ref=gath.at[slot, rows, cols], dst_ref=gath.at[6, rows, cols],
            send_sem=s_opp.at[n, h, kind], recv_sem=recv.at[sem, h, kind], **to(peer))

    def opp_landed(n, h, kind):
        cols = att_cols if kind else act_cols
        part = gath.at[6, pl.ds(h * hb + n * qtr, qtr), cols]
        return pltpu.make_async_remote_copy(
            src_ref=part, dst_ref=part, send_sem=s_opp.at[n, h, kind], recv_sem=recv.at[(6, 2 * nx)[n], h, kind], **to(other))

    def par_send(slot, h, kind):
        cols = att_cols if kind else act_cols
        return pltpu.make_async_remote_copy(
            src_ref=gath.at[slot, pl.ds(h * hb, hb), cols], dst_ref=gath.at[slot + 1, pl.ds(h * hb, hb), cols],
            send_sem=s_par.at[slot // 2 - 1, h, kind], recv_sem=recv.at[slot + 1, h, kind], **to(other))

    def landed(slot, h, kind):
        cols = att_cols if kind else act_cols
        part = gath.at[slot, pl.ds(h * hb, hb), cols]
        return pltpu.make_async_remote_copy(
            src_ref=part, dst_ref=part, send_sem=s_own.at[0, 0, 0], recv_sem=recv.at[slot, h, kind], **to(other))

    locals_ = [pltpu.make_async_copy(act_ref, gath.at[0, :, act_cols], c_loc.at[0]),
               pltpu.make_async_copy(wo_ref, w2.at[att_cols, :], c_loc.at[1]),
               pltpu.make_async_copy(wd_ref, w2.at[act_cols, :], c_loc.at[2]),
               pltpu.make_async_copy(x_hbm, x_ref, c_loc.at[3])]
    qkv_copy = pltpu.make_async_copy(qkv_hbm, qkv_ref, c_loc.at[4])
    qkv_copy.start()

    ctx = kc_ref.shape[1]
    cs = kbuf.shape[1]
    n_chunks = ctx // cs

    def cache_copy(side, idx):
        ref, buf = ((kc_ref, kbuf), (vc_ref, vbuf))[side]
        slot = lax.rem(idx, 2)
        return pltpu.make_async_copy(ref.at[idx // n_chunks, pl.ds(lax.rem(idx, n_chunks) * cs, cs)], buf.at[slot],
                                     kv_loc.at[side, slot])

    for side in range(2):
        cache_copy(side, 0).start()

    barrier = pltpu.get_barrier_semaphore()
    for peer in (other, right, left):
        pl.semaphore_signal(barrier, inc=1, **to(peer))
    for peer in (p1, p2):
        pl.semaphore_signal(barrier, inc=1, **to_y(peer))
    pl.semaphore_wait(barrier, 5)

    for h in range(2):
        for n in range(3):
            own_send(n, h, 0).start()
    for copy in locals_:
        copy.start()

    kv_wide = kv_heads * head
    gbuf[...] = jnp.zeros(gbuf.shape, F32)
    gbuf[0:heads, 0:head] = qgain_ref[...].astype(F32)
    gbuf[heads:heads + kv_heads, 0:head] = kgain_ref[...].astype(F32)
    gain_t = jnp.transpose(gbuf[...])
    gswap_t = swap_pairs(gain_t)
    line = lax.broadcasted_iota(jnp.int32, (head, rb), 0)
    odd = lax.rem(line, 2)
    inv_freq = jnp.exp((line - odd).astype(F32) * (-math.log(ROPE_THETA) / head))
    angles = inv_freq * pos_ref[...].astype(F32)
    cos_a = jnp.cos(angles)
    sin_a = jnp.sin(angles) * (2 * odd - 1).astype(F32)
    qkv_copy.wait()
    qkv_t = jnp.transpose(qkv_ref[...].astype(F32))
    swap_t = swap_pairs(qkv_t[:natt + kv_wide])
    for n in range(heads + kv_heads):
        own = slice(n * head, (n + 1) * head)
        one, two = qkv_t[own], swap_t[own]
        mean = jnp.mean(one, axis=0, keepdims=True)
        centred = one - mean
        scale = lax.rsqrt(jnp.mean(centred * centred, axis=0, keepdims=True) + NORM_EPS)
        turned = (centred * scale * gain_t[:head, n:n + 1] * cos_a
                  + (two - mean) * scale * gswap_t[:head, n:n + 1] * sin_a)
        turned = turned.astype(BF16)
        if n < heads:
            qt[n] = turned.astype(F32)
        else:
            k_out[n - heads] = turned
            kt[n - heads] = turned.astype(F32)
    for n in range(kv_heads):
        one = qkv_t[natt + kv_wide + n * head:natt + kv_wide + (n + 1) * head]
        vt[n] = one
        v_out[n] = one.astype(BF16)

    new_leave = (pltpu.make_async_copy(k_out, k_hbm, o_sem.at[0]), pltpu.make_async_copy(v_out, v_hbm, o_sem.at[1]))
    for copy in new_leave:
        copy.start()

    score_scale = head ** -0.5
    db = 16

    def attend_head(kv, carry):
        first = kv * group

        def score_chunk(c, inner):
            idx = kv * n_chunks + c
            slot = lax.rem(idx, 2)
            cache_copy(0, idx).wait()

            @pl.when(idx < kv_heads * n_chunks - 1)
            def _():
                cache_copy(0, idx + 1).start()

            def score(s, deep):
                keys = kbuf[slot, s].astype(F32)
                sc[c * cs + s] = jnp.concatenate(
                    [jnp.sum(qt[first + j] * keys, axis=0, keepdims=True) for j in range(group)], axis=0)
                return deep

            return lax.fori_loop(0, cs, score, inner)

        lax.fori_loop(0, n_chunks, score_chunk, 0)
        k_one = kt[kv]
        s_one = jnp.concatenate([jnp.sum(qt[first + j] * k_one, axis=0, keepdims=True) for j in range(group)], axis=0) * score_scale
        scores = sc[...] * score_scale
        at = lax.broadcasted_iota(jnp.int32, scores.shape, 0)
        scores = jnp.where(at < pos_ref[...][None], scores, -1e30)
        top = jnp.maximum(jnp.max(scores, axis=0), s_one)
        probs = jnp.exp(scores - top[None])
        p_one = jnp.exp(s_one - top)
        denom = jnp.sum(probs, axis=0) + p_one
        sc[...] = probs.astype(BF16).astype(F32)
        v_one = vt[kv]
        for j in range(group):
            oc[j] = p_one[j:j + 1] * v_one

        def value_chunk(c, inner):
            idx = kv * n_chunks + c
            slot = lax.rem(idx, 2)
            cache_copy(1, idx).wait()

            @pl.when(idx < kv_heads * n_chunks - 1)
            def _():
                cache_copy(1, idx + 1).start()

            def value(b, deep):
                lines = pl.ds(pl.multiple_of(b * db, db), db)
                sums = [oc[j, lines, :] for j in range(group)]
                for s in range(cs):
                    vals = vbuf[slot, s, lines, :].astype(F32)
                    for j in range(group):
                        sums[j] = sums[j] + sc[c * cs + s, j:j + 1, :] * vals
                for j in range(group):
                    oc[j, lines, :] = sums[j]
                return deep

            return lax.fori_loop(0, head // db, value, inner)

        lax.fori_loop(0, n_chunks, value_chunk, 0)
        for j in range(group):
            lines = pl.ds(pl.multiple_of((first + j) * head, 8), head)
            ot[lines, :] = oc[j] / denom[j:j + 1]
        return carry

    lax.fori_loop(0, kv_heads, attend_head, 0)
    gath[0, :, 0:natt] = jnp.transpose(ot[...]).astype(BF16)
    for h in range(2):
        for n in range(3):
            own_send(n, h, 1).start()
    for copy in locals_:
        copy.wait()

    def block_rows(place, j):
        off = place + (place // 2) * (5 - 2 * place)
        who = core + j * (1 - 2 * core)
        return (lax.rem(xi + off, nx) * 2 + who) * rb

    groups = [(place, 0, rb) for place in range(nx - 1)] + [(nx - 1, 0, hb), (nx - 1, hb, hb)]

    def aligned(start, size):
        return pl.ds(pl.multiple_of(start, size), size)

    def y1(g, j):
        place, row0, size = groups[g]
        i = 2 * place + j
        return pltpu.make_async_remote_copy(
            src_ref=pb.at[i, aligned(row0 + (1 - b1) * (size // 2), size // 2), :], dst_ref=r1.at[i, pl.ds(row0 // 2, size // 2), :],
            send_sem=y1s.at[2 * g + j], recv_sem=y1r.at[2 * g + j], **to_y(p1))

    def y2(g, j):
        place, row0, size = groups[g]
        i = 2 * place + j
        rows = pl.ds(row0 // 4, size // 4)
        return pltpu.make_async_remote_copy(
            src_ref=mq.at[i, rows, :], dst_ref=r2.at[i, rows, :],
            send_sem=y2s.at[2 * g + j], recv_sem=y2r.at[2 * g + j], **to_y(p2))

    def y3(g, j, mine):
        place, row0, size = groups[g]
        quarter = b2 if mine else 1 - b2
        start = block_rows(place, j) + row0 + b1 * (size // 2) + quarter * (size // 4)
        rows = out_ref.at[aligned(start, size // 4), :]
        return pltpu.make_async_remote_copy(
            src_ref=rows, dst_ref=rows, send_sem=y3s.at[2 * g + j], recv_sem=y3r.at[2 * g + j], **to_y(p2))

    def y4(g, j, mine):
        place, row0, size = groups[g]
        half = b1 if mine else 1 - b1
        rows = out_ref.at[aligned(block_rows(place, j) + row0 + half * (size // 2), size // 2), :]
        return pltpu.make_async_remote_copy(
            src_ref=rows, dst_ref=rows, send_sem=y4s.at[2 * g + j], recv_sem=y4r.at[2 * g + j], **to_y(p1))

    def product(g, kinds=(0, 1)):
        place, row0, size = groups[g]
        rows = pl.ds(row0, size)
        if len(kinds) == 2:
            cols = slice(None)
        else:
            cols = att_cols if kinds[0] else act_cols

        def body(j, carry):
            i = 2 * place + j

            @pl.when(j == 1)
            def _():
                for kind in kinds:
                    for h in range(row0 // hb, (row0 + size) // hb):
                        landed(2 * place + 1, h, kind).wait_recv()

            part = jnp.dot(gath[i, rows, cols], w2[cols, :], preferred_element_type=F32)
            if kinds == (1,):
                part = part + mf[i, rows, :]
            mf[i, rows, :] = part
            if 1 in kinds:
                pb[i, rows, :] = part.astype(BF16)
                y1(g, j).start()
            return carry

        lax.fori_loop(0, 2, body, 0)

    def stage2(g):
        place, row0, size = groups[g]
        for j in range(2):
            i = 2 * place + j
            y1(g, j).wait_recv()
            rows = aligned(row0 + b1 * (size // 2) + (1 - b2) * (size // 4), size // 4)
            sub = aligned(row0 // 2 + (1 - b2) * (size // 4), size // 4)
            mq[i, row0 // 4:(row0 + size) // 4, :] = (mf[i, rows, :] + r1[i, sub, :].astype(F32)).astype(BF16)
            y2(g, j).start()

    def stage3(g):
        place, row0, size = groups[g]
        for j in range(2):
            i = 2 * place + j
            y2(g, j).wait_recv()
            rows = aligned(row0 + b1 * (size // 2) + b2 * (size // 4), size // 4)
            sub = aligned(row0 // 2 + b2 * (size // 4), size // 4)
            total = mf[i, rows, :] + r1[i, sub, :].astype(F32) + r2[i, row0 // 4:(row0 + size) // 4, :].astype(F32)
            rows = aligned(block_rows(place, j) + row0 + b1 * (size // 2) + b2 * (size // 4), size // 4)
            out_ref[rows, :] = (x_ref[rows, :].astype(F32) + total).astype(BF16)
            y3(g, j, True).start()

    def stage4(g):
        for j in range(2):
            y3(g, j, False).wait_recv()
            y4(g, j, True).start()

    def leave(g, j):
        place, row0, size = groups[g]
        rows = aligned(block_rows(place, j) + row0, size)
        return pltpu.make_async_copy(out_ref.at[rows, :], out_hbm.at[rows, :], o_sem.at[2 + 2 * g + j])

    def settled(g):
        for j in range(2):
            y4(g, j, False).wait_recv()
            leave(g, j).start()

    def near_landed(kind):
        for slot in (2, 4):
            for h in range(2):
                landed(slot, h, kind).wait_recv()
        if kind == 0:
            forwards = ((0, 0),)
        else:
            forwards = ((0, 1), (1, 0), (1, 1))
        for h, k in forwards:
            for n in range(2):
                opp_send(n, h, k).start()
        for slot in (2, 4):
            for h in range(2):
                par_send(slot, h, kind).start()

    def far_landed(h, kind):
        for n in range(2):
            opp_landed(n, h, kind).wait_recv()
        par_send(6, h, kind).start()

    product(0)
    stage2(0)
    near_landed(0)
    stage3(0)
    near_landed(1)
    stage4(0)
    product(1)
    product(2)
    stage2(1)
    stage2(2)
    far_landed(0, 0)
    far_landed(0, 1)
    stage3(1)
    stage3(2)
    product(3)
    stage4(1)
    stage4(2)
    stage2(3)
    stage3(3)
    far_landed(1, 0)
    product(4, (0,))
    for g in range(nx - 1):
        settled(g)
    far_landed(1, 1)
    product(4, (1,))
    stage4(3)
    stage2(4)
    stage3(4)
    stage4(4)

    for g in range(nx - 1, len(groups)):
        settled(g)
    for g in range(len(groups)):
        for j in range(2):
            leave(g, j).wait()
            y1(g, j).wait_send()
            y2(g, j).wait_send()
            y3(g, j, True).wait_send()
            y4(g, j, True).wait_send()
    for copy in new_leave:
        copy.wait()
    for kind in range(2):
        for h in range(2):
            for n in range(3):
                own_send(n, h, kind).wait_send()
            for slot in (2, 4, 6):
                par_send(slot, h, kind).wait_send()
            for n in range(2):
                opp_send(n, h, kind).wait_send()


def finish(nx, ny, act, qkv, k_cache, v_cache, positions, q_gain, k_gain, w_out, w_down, x_in):
    rb, nf = act.shape
    kv_heads, ctx, head = k_cache.shape[:3]
    natt, wcols = w_out.shape
    heads = natt // head
    group = heads // kv_heads
    cs = 16
    vmem = pl.BlockSpec(memory_space=pltpu.VMEM)
    hbm = pl.BlockSpec(memory_space=ANY)
    dma = pltpu.SemaphoreType.DMA
    new = jax.ShapeDtypeStruct((kv_heads, head, rb), BF16)
    return pl.pallas_call(
        functools.partial(finish_kernel, nx, ny, heads, kv_heads),
        out_shape=(jax.ShapeDtypeStruct(x_in.shape, BF16), new, new),
        in_specs=[hbm, hbm, hbm, hbm, vmem, vmem, vmem, hbm, hbm, hbm],
        out_specs=(hbm, hbm, hbm),
        scratch_shapes=[
            pltpu.VMEM(x_in.shape, BF16),
            pltpu.VMEM(new.shape, BF16),
            pltpu.VMEM(new.shape, BF16),
            dma((2 + 4 * nx,)),
            pltpu.VMEM(qkv.shape, BF16),
            pltpu.VMEM(x_in.shape, BF16),
            pltpu.VMEM((128, pl.cdiv(head, 128) * 128), F32),
            pltpu.VMEM((2 * nx, rb, natt + nf), BF16),
            pltpu.VMEM((natt + nf, wcols), BF16),
            pltpu.VMEM((heads, head, rb), F32),
            pltpu.VMEM((kv_heads, head, rb), F32),
            pltpu.VMEM((kv_heads, head, rb), F32),
            pltpu.VMEM((ctx, group, rb), F32),
            pltpu.VMEM((group, head, rb), F32),
            pltpu.VMEM((natt, rb), F32),
            pltpu.VMEM((2, cs, head, rb), BF16),
            pltpu.VMEM((2, cs, head, rb), BF16),
            pltpu.VMEM((2 * nx, rb, wcols), BF16),
            pltpu.VMEM((2 * nx, rb // 2, wcols), BF16),
            pltpu.VMEM((2 * nx, rb, wcols), F32),
            pltpu.VMEM((2 * nx, rb // 4, wcols), BF16),
            pltpu.VMEM((2 * nx, rb // 4, wcols), BF16),
            dma((5,)),
            dma((2, 2)),
            dma((3, 2, 2)),
            dma((2, 2, 2)),
            dma((3, 2, 2)),
            dma((2 * nx + 1, 2, 2)),
        ] + [dma((2 * nx + 2,))] * 8,
        compiler_params=pltpu.CompilerParams(collective_id=1, has_side_effects=True, vmem_limit_bytes=VMEM_LIMIT),
        name='finish',
    )(act, qkv, k_cache, v_cache, positions, q_gain, k_gain, w_out, w_down, x_in)


def settle_kernel(n_parts, x_ref, k_ref, v_ref, x_out, k_out, v_out, xbuf, kbuf, vbuf, sem_in, sem_out):
    rows = x_ref.shape[0] // n_parts
    moves = [(x_ref.at[pl.ds(n * rows, rows)], xbuf.at[pl.ds(n * rows, rows)], x_out.at[pl.ds(n * rows, rows)]) for n in range(n_parts)]
    moves += [(k_ref, kbuf, k_out), (v_ref, vbuf, v_out)]
    for n, (src, mid, _) in enumerate(moves):
        pltpu.make_async_copy(src, mid, sem_in.at[n]).start()
    for n, (src, mid, dst) in enumerate(moves):
        pltpu.make_async_copy(src, mid, sem_in.at[n]).wait()
        pltpu.make_async_copy(mid, dst, sem_out.at[n]).start()
    for n, (_, mid, dst) in enumerate(moves):
        pltpu.make_async_copy(mid, dst, sem_out.at[n]).wait()


def settle(x_out, k_t, v_t):
    n_parts = 4
    hbm = pl.BlockSpec(memory_space=ANY)
    arrays = (x_out, k_t, v_t)
    return pl.pallas_call(
        functools.partial(settle_kernel, n_parts),
        out_shape=tuple(jax.ShapeDtypeStruct(a.shape, a.dtype) for a in arrays),
        in_specs=[hbm] * 3,
        out_specs=(hbm,) * 3,
        scratch_shapes=[pltpu.VMEM(a.shape, a.dtype) for a in arrays] + [pltpu.SemaphoreType.DMA((n_parts + 2,))] * 2,
        name='settle',
    )(*arrays)


def solution(mesh):
    dm_size = mesh.shape['dm']
    nx = dm_size // 2
    x_spec = P('dp', 'dm')
    row_spec = P(('dp', 'dm'))
    cache_spec = P(('dp', 'dm'), 'tp', None, None)
    new_spec = P(('dp', 'dm'), 'tp', None)
    hid_tp = P('dm', 'tp')
    tp_hid = P('tp', 'dm')
    head_spec = P('tp', None)

    def device_step(x_in, positions, k_cache, v_cache, ln_gain, w_q, w_k, w_v, w_gate, w_up, q_gain, k_gain, w_out, w_down):
        qkv, act = project(nx, x_in, ln_gain, w_q, w_k.T, w_v.T, w_gate, w_up)
        x_out, k_t, v_t = settle(*finish(
            nx, mesh.shape['tp'], act, qkv, jnp.transpose(k_cache, (1, 2, 3, 0)), jnp.transpose(v_cache, (1, 2, 3, 0)),
            positions[None, :], q_gain, k_gain, w_out, w_down, x_in))
        k_new = jnp.transpose(k_t, (2, 0, 1))
        v_new = jnp.transpose(v_t, (2, 0, 1))
        return x_out, k_new, v_new

    return jax.shard_map(
        device_step,
        mesh=mesh,
        in_specs=(x_spec, row_spec, cache_spec, cache_spec, P('dm'), hid_tp, hid_tp, hid_tp, hid_tp, hid_tp, head_spec, head_spec, tp_hid, tp_hid),
        out_specs=(x_spec, new_spec, new_spec),
        check_vma=False,
    )
```

```python
import functools
import math

import jax
import jax.numpy as jnp
from jax import lax
from jax.experimental import pallas as pl
from jax.experimental.pallas import tpu as pltpu
from jax.sharding import PartitionSpec as P

NORM_EPS = 1e-5
ROPE_THETA = 75000000.0
MESH = pl.DeviceIdType.MESH
BF16 = jnp.bfloat16
F32 = jnp.float32
ANY = pl.ANY
VMEM_LIMIT = 66 * 1024 * 1000 - 1024 * 600


def project_kernel(nx, nload, ntile, x_ref, gain_ref, wq_ref, wk_ref, wv_ref, wg_ref, wu_ref,
                   qkv_out, act_out,
                   xbuf, gain, stat, bq, bkv, bg, bu, rq, rkv, rg, lq, lkv, lu, qkv_buf, act_buf,
                   o_sem, x_loc, x_snd, x_rcv, t_snd, t_rcv, w_loc, w_snd, w_rcv, r_snd, r_rcv):
    dm = lax.axis_index('dm')
    xi = dm // 2
    core = lax.rem(dm, 2)
    other = 2 * xi + 1 - core
    right = lax.rem(xi + 1, nx) * 2 + core
    left = lax.rem(xi + nx - 1, nx) * 2 + core
    rb = xbuf.shape[1]
    hb = rb // 2
    hid = x_ref.shape[1]
    tw = wg_ref.shape[1] // ntile
    lw = wg_ref.shape[1] // nload
    per = ntile // nload

    every = slice(None)
    kw = wk_ref.shape[0]
    pieces = [(wq_ref, bq, 0, every), (wk_ref, bkv, 1, pl.ds(0, kw)), (wv_ref, bkv, 1, pl.ds(kw, kw))]
    for n in range(nload):
        pieces.append((wg_ref, bg, 0, pl.ds(n * lw, lw)))
        pieces.append((wu_ref, bu, 0, pl.ds(n * lw, lw)))

    def x_local(j):
        return pltpu.make_async_copy(
            x_ref.at[pl.ds((2 * j + core) * rb, rb), :], xbuf.at[j, :, pl.ds(0, hid)], x_loc.at[j])

    def x_remote(j):
        return pltpu.make_async_remote_copy(
            src_ref=x_ref.at[pl.ds((2 * j + 1 - core) * rb, rb), :], dst_ref=xbuf.at[j, :, pl.ds(hid, hid)],
            send_sem=x_snd.at[j], recv_sem=x_rcv.at[j], device_id={'dm': other}, device_id_type=MESH)

    def w_place(n, start):
        _, dst, side, cut = pieces[n]
        return dst.at[cut, pl.ds(start, hid)] if side else dst.at[pl.ds(start, hid), cut]

    def w_source(n):
        src, _, side, cut = pieces[n]
        return src if side else src.at[:, cut]

    def w_local(n):
        return pltpu.make_async_copy(w_source(n), w_place(n, 0), w_loc.at[n])

    def w_remote(n):
        return pltpu.make_async_remote_copy(
            src_ref=w_source(n), dst_ref=w_place(n, hid), send_sem=w_snd.at[n], recv_sem=w_rcv.at[n],
            device_id={'dm': other}, device_id_type=MESH)

    def g_remote():
        return pltpu.make_async_remote_copy(
            src_ref=gain.at[:, pl.ds(0, hid)], dst_ref=gain.at[:, pl.ds(hid, hid)], send_sem=x_snd.at[nx], recv_sem=x_rcv.at[nx],
            device_id={'dm': other}, device_id_type=MESH)

    def t_remote(d):
        return pltpu.make_async_remote_copy(
            src_ref=stat.at[0], dst_ref=stat.at[d], send_sem=t_snd.at[d - 1], recv_sem=t_rcv.at[d - 1],
            device_id={'dm': lax.rem(xi + d, nx) * 2 + core}, device_id_type=MESH)

    gain[:, 0:hid] = jnp.broadcast_to(gain_ref[...].astype(F32)[None, :], (8, hid))
    for j in range(nx):
        x_local(j).start()
    for n in range(len(pieces)):
        w_local(n).start()

    barrier = pltpu.get_barrier_semaphore()
    pl.semaphore_signal(barrier, inc=1, device_id={'dm': other}, device_id_type=MESH)
    for d in range(1, nx):
        pl.semaphore_signal(barrier, inc=1, device_id={'dm': lax.rem(xi + d, nx) * 2 + core}, device_id_type=MESH)
    pl.semaphore_wait(barrier, nx)

    for j in range(nx):
        x_remote(j).start()
    g_remote().start()
    w_remote(0).start()

    for ref in (rq, rkv, rg, lq, lkv, lu):
        ref[0] = jnp.zeros(ref.shape[1:], ref.dtype)

    lane = lax.broadcasted_iota(jnp.int32, (rb, 128), 1)
    both = jnp.zeros((rb, 128), F32)
    for j in range(nx):
        x_local(j).wait()
        x_remote(j).wait()
        values = xbuf[j].astype(F32)
        mean = jnp.mean(values, axis=1, keepdims=True)
        centred = values - mean
        both = jnp.where(lane == 2 * j, mean, both)
        both = jnp.where(lane == 2 * j + 1, jnp.sum(centred * centred, axis=1, keepdims=True), both)
    for n in range(1, 5):
        w_remote(n).start()
    stat[0] = jnp.transpose(both)[:2 * nx]
    for d in range(1, nx):
        t_remote(d).start()
    g_remote().wait()
    for d in range(1, nx):
        t_remote(d).wait()
    parts = [stat[d] for d in range(nx)]
    total = sum(parts[1:], parts[0])
    row_mean = total / nx
    spread = sum([(p - row_mean) * (p - row_mean) for p in parts[1:]], (parts[0] - row_mean) * (parts[0] - row_mean))
    variance = (total + 2 * hid * pltpu.roll(spread, 1, 0)) / (2 * hid * nx)
    line = lax.broadcasted_iota(jnp.int32, total.shape, 0)
    both = jnp.where(lax.rem(line, 2) == 0, row_mean, lax.rsqrt(variance + NORM_EPS))
    both = jnp.transpose(jnp.concatenate([both, jnp.zeros((128 - 2 * nx, rb), F32)], axis=0))
    for j in range(nx):
        values = xbuf[j].astype(F32) - both[:, 2 * j:2 * j + 1]
        xbuf[j] = (values * both[:, 2 * j + 1:2 * j + 2] * gain[0:1, :]).astype(BF16)

    def hop(d, t, s, slot, cols):
        nxt = jnp.minimum(s + 1, nx - 1)
        return pltpu.make_async_remote_copy(
            src_ref=slot.at[s, :, cols], dst_ref=slot.at[nxt, :, cols],
            send_sem=r_snd.at[d, t, s], recv_sem=r_rcv.at[d, t, nxt],
            device_id={'dm': left if d else right}, device_id_type=MESH)

    def arrived(d, t, s, slot, cols):
        return pltpu.make_async_remote_copy(
            src_ref=slot.at[s, :, cols], dst_ref=slot.at[s, :, cols],
            send_sem=r_snd.at[d, t, s], recv_sem=r_rcv.at[d, t, s],
            device_id={'dm': left if d else right}, device_id_type=MESH)

    def partial(d, s, weight, w_cols):
        row = lax.rem(xi + 1 + s, nx) if d else lax.rem(xi + 2 * nx - 1 - s, nx)
        if w_cols is None:
            return lax.dot_general(xbuf[row, d * hb:(d + 1) * hb, :], weight[...], (((1,), (1,)), ((), ())),
                                   preferred_element_type=F32)
        return jnp.dot(xbuf[row], weight[:, w_cols], preferred_element_type=F32)

    def pass_on(part, d, t, s, slot, cols):
        @pl.when(s > 0)
        def _():
            arrived(d, t, s, slot, cols).wait_recv()

        slot[s, :, cols] = (part + slot[s, :, cols].astype(F32)).astype(BF16)

        @pl.when(s < nx - 1)
        def _():
            hop(d, t, s, slot, cols).start()

    def wait_piece(n):
        w_local(n).wait()
        w_remote(n).wait()

    half = rq.shape[2]
    qkv_leave = pltpu.make_async_copy(qkv_buf, qkv_out, o_sem.at[ntile])

    def act_leave(t):
        cols = pl.ds(pl.multiple_of(t * tw, 128), tw)
        return pltpu.make_async_copy(act_buf.at[:, cols], act_out.at[:, cols], o_sem.at[t])


    def step(s, carry):
        @pl.when(s == 0)
        def _():
            wait_piece(0)
            for n in range(5, len(pieces)):
                if (n - 3) // 2 == 1:
                    w_remote(n).start()

        pass_on(partial(0, s, bq, pl.ds(0, half)), 0, 0, s, rq, pl.ds(0, half))
        pass_on(partial(1, s, bq, pl.ds(half, half)), 1, 0, s, lq, pl.ds(0, half))

        @pl.when(s == 0)
        def _():
            wait_piece(1)
            wait_piece(2)

        pass_on(partial(0, s, bkv, None), 0, 1, s, rkv, pl.ds(0, 2 * kw))
        pass_on(partial(1, s, bkv, None), 1, 1, s, lkv, pl.ds(0, 2 * kw))

        @pl.when(s == nx - 1)
        def _():
            qkv_buf[:, :half] = rq[nx - 1]
            qkv_buf[:, half:2 * half] = lq[nx - 1]
            qkv_buf[:hb, 2 * half:] = rkv[nx - 1]
            qkv_buf[hb:, 2 * half:] = lkv[nx - 1]
            qkv_leave.start()

        def mlp(t, inner):
            for now in range(nload):
                @pl.when((s == 0) & (t == now * per))
                def _():
                    wait_piece(3 + 2 * now)
                    wait_piece(4 + 2 * now)
                    if 5 + 2 * now + 2 < len(pieces):
                        w_remote(7 + 2 * now).start()
                        w_remote(8 + 2 * now).start()

            cols = pl.ds(pl.multiple_of(t * tw, 128), tw)
            part_g = partial(0, s, bg, cols)
            part_u = partial(1, s, bu, cols)
            pass_on(part_g, 0, 2 + t, s, rg, cols)
            pass_on(part_u, 1, 2 + t, s, lu, cols)

            @pl.when(s == nx - 1)
            def _():
                gate = rg[nx - 1, :, cols].astype(F32)
                up = lu[nx - 1, :, cols].astype(F32)
                act_buf[:, cols] = (gate / (1.0 + jnp.exp(-gate)) * up).astype(BF16)
                act_leave(t).start()

            return inner

        return lax.fori_loop(0, ntile, mlp, carry)

    lax.fori_loop(0, nx, step, 0)
    def sent(s, carry):
        hop(0, 0, s, rq, pl.ds(0, half)).wait_send()
        hop(1, 0, s, lq, pl.ds(0, half)).wait_send()
        hop(0, 1, s, rkv, pl.ds(0, 2 * kw)).wait_send()
        hop(1, 1, s, lkv, pl.ds(0, 2 * kw)).wait_send()
        def sent_mlp(t, inner):
            cols = pl.ds(pl.multiple_of(t * tw, 128), tw)
            hop(0, 2 + t, s, rg, cols).wait_send()
            hop(1, 2 + t, s, lu, cols).wait_send()
            return inner

        return lax.fori_loop(0, ntile, sent_mlp, carry)

    lax.fori_loop(0, nx - 1, sent, 0)
    qkv_leave.wait()

    def left_all(t, carry):
        act_leave(t).wait()
        return carry

    lax.fori_loop(0, ntile, left_all, 0)


def project(nx, x_in, gain, w_q, w_k_t, w_v_t, w_gate, w_up):
    rows, hid = x_in.shape
    rb = rows // (2 * nx)
    nq, nk, nf = w_q.shape[1], w_k_t.shape[0], w_gate.shape[1]
    nload, ntile = 3, 9
    npiece = 3 + 2 * nload
    vmem = pl.BlockSpec(memory_space=pltpu.VMEM)
    dma = pltpu.SemaphoreType.DMA
    return pl.pallas_call(
        functools.partial(project_kernel, nx, nload, ntile),
        out_shape=(jax.ShapeDtypeStruct((rb, nq + 2 * nk), BF16), jax.ShapeDtypeStruct((rb, nf), BF16)),
        in_specs=[pl.BlockSpec(memory_space=ANY), vmem] + [pl.BlockSpec(memory_space=ANY)] * 5,
        out_specs=(pl.BlockSpec(memory_space=ANY),) * 2,
        scratch_shapes=[
            pltpu.VMEM((nx, rb, 2 * hid), BF16),
            pltpu.VMEM((8, 2 * hid), F32),
            pltpu.VMEM((nx, 2 * nx, rb), F32),
            pltpu.VMEM((2 * hid, nq), BF16),
            pltpu.VMEM((2 * nk, 2 * hid), BF16),
            pltpu.VMEM((2 * hid, nf), BF16),
            pltpu.VMEM((2 * hid, nf), BF16),
            pltpu.VMEM((nx, rb, nq // 2), BF16),
            pltpu.VMEM((nx, rb // 2, 2 * nk), BF16),
            pltpu.VMEM((nx, rb, nf), BF16),
            pltpu.VMEM((nx, rb, nq // 2), BF16),
            pltpu.VMEM((nx, rb // 2, 2 * nk), BF16),
            pltpu.VMEM((nx, rb, nf), BF16),
            pltpu.VMEM((rb, nq + 2 * nk), BF16),
            pltpu.VMEM((rb, nf), BF16),
            dma((ntile + 1,)),
            dma((nx,)),
            dma((nx + 1,)),
            dma((nx + 1,)),
            dma((nx - 1,)),
            dma((nx - 1,)),
            dma((npiece,)),
            dma((npiece,)),
            dma((npiece,)),
            dma((2, 2 + ntile, nx)),
            dma((2, 2 + ntile, nx)),
        ],
        compiler_params=pltpu.CompilerParams(collective_id=0, has_side_effects=True, vmem_limit_bytes=VMEM_LIMIT),
        name='project',
    )(x_in, gain, w_q, w_k_t, w_v_t, w_gate, w_up)


def swap_pairs(v):
    length = v.shape[0]
    line = lax.broadcasted_iota(jnp.int32, v.shape, 0)
    return jnp.where(lax.rem(line, 2) == 0, pltpu.roll(v, length - 1, 0), pltpu.roll(v, 1, 0))


def finish_kernel(nx, ny, heads, kv_heads, act_ref, qkv_hbm, kc_ref, vc_ref, pos_ref, qgain_ref, kgain_ref,
                  wo_ref, wd_ref, x_hbm, out_hbm, k_hbm, v_hbm,
                  out_ref, k_out, v_out, o_sem, qkv_ref, x_ref, gbuf, gath, w2, qt, kt, vt, sc, oc, ot, kbuf, vbuf, pb, r1, mf, mq, r2,
                  c_loc, kv_loc, s_own, s_opp, s_par, recv, y1s, y1r, y2s, y2r, y3s, y3r, y4s, y4r, y5s, y5r):
    dm = lax.axis_index('dm')
    y = lax.axis_index('tp')
    xi = dm // 2
    core = lax.rem(dm, 2)
    other = 2 * xi + 1 - core
    right = lax.rem(xi + 1, nx) * 2 + core
    left = lax.rem(xi + nx - 1, nx) * 2 + core
    nf = act_ref.shape[1]
    rb = act_ref.shape[0]
    hb, qtr = rb // 2, rb // 4
    head = qgain_ref.shape[1]
    natt = heads * head
    group = heads // kv_heads
    flip, mirror = y + 1 - 2 * lax.rem(y, 2), ny - 1 - y
    p1 = flip + core * (mirror - flip)
    p2 = mirror + core * (flip - mirror)
    p3 = lax.rem(y + 2, ny)
    bit_a, bit_b, bit_c = lax.rem((y + 1) // 2, 2), y // 2, lax.rem(y, 2)
    b1 = bit_a + core * (bit_b - bit_a)
    b2 = bit_b + core * (bit_c - bit_b)
    q1 = b2 + core * (1 - 2 * b2)

    act_cols, att_cols = pl.ds(natt, nf), pl.ds(0, natt)

    def to(peer):
        return dict(device_id={'dm': peer}, device_id_type=MESH)

    def to_y(peer):
        return dict(device_id={'tp': peer}, device_id_type=MESH)

    def own_send(n, h, kind):
        peer, slot = ((right, 4), (left, 2), (other, 1))[n]
        cols = att_cols if kind else act_cols
        src = gath.at[0, pl.ds(h * hb, hb), cols] if kind else act_ref.at[pl.ds(h * hb, hb), :]
        return pltpu.make_async_remote_copy(
            src_ref=src, dst_ref=gath.at[slot, pl.ds(h * hb, hb), cols],
            send_sem=s_own.at[n, h, kind], recv_sem=recv.at[slot, h, kind], **to(peer))

    def opp_send(n, h, kind):
        peer, slot, sem = ((right, 4, 6), (left, 2, 2 * nx))[n]
        cols = att_cols if kind else act_cols
        rows = pl.ds(h * hb + n * qtr, qtr)
        return pltpu.make_async_remote_copy(
            src_ref=gath.at[slot, rows, cols], dst_ref=gath.at[6, rows, cols],
            send_sem=s_opp.at[n, h, kind], recv_sem=recv.at[sem, h, kind], **to(peer))

    def opp_landed(n, h, kind):
        cols = att_cols if kind else act_cols
        part = gath.at[6, pl.ds(h * hb + n * qtr, qtr), cols]
        return pltpu.make_async_remote_copy(
            src_ref=part, dst_ref=part, send_sem=s_opp.at[n, h, kind], recv_sem=recv.at[(6, 2 * nx)[n], h, kind], **to(other))

    def par_send(slot, h, kind):
        cols = att_cols if kind else act_cols
        return pltpu.make_async_remote_copy(
            src_ref=gath.at[slot, pl.ds(h * hb, hb), cols], dst_ref=gath.at[slot + 1, pl.ds(h * hb, hb), cols],
            send_sem=s_par.at[slot // 2 - 1, h, kind], recv_sem=recv.at[slot + 1, h, kind], **to(other))

    def landed(slot, h, kind):
        cols = att_cols if kind else act_cols
        part = gath.at[slot, pl.ds(h * hb, hb), cols]
        return pltpu.make_async_remote_copy(
            src_ref=part, dst_ref=part, send_sem=s_own.at[0, 0, 0], recv_sem=recv.at[slot, h, kind], **to(other))

    locals_ = [pltpu.make_async_copy(act_ref, gath.at[0, :, act_cols], c_loc.at[0]),
               pltpu.make_async_copy(wo_ref, w2.at[att_cols, :], c_loc.at[1]),
               pltpu.make_async_copy(wd_ref, w2.at[act_cols, :], c_loc.at[2]),
               pltpu.make_async_copy(x_hbm, x_ref, c_loc.at[3])]
    qkv_copy = pltpu.make_async_copy(qkv_hbm, qkv_ref, c_loc.at[4])
    qkv_copy.start()

    ctx = kc_ref.shape[1]
    cs = kbuf.shape[1]
    n_chunks = ctx // cs

    def cache_copy(side, idx):
        ref, buf = ((kc_ref, kbuf), (vc_ref, vbuf))[side]
        slot = lax.rem(idx, 2)
        return pltpu.make_async_copy(ref.at[idx // n_chunks, pl.ds(lax.rem(idx, n_chunks) * cs, cs)], buf.at[slot],
                                     kv_loc.at[side, slot])

    for side in range(2):
        cache_copy(side, 0).start()

    barrier = pltpu.get_barrier_semaphore()
    for peer in (other, right, left):
        pl.semaphore_signal(barrier, inc=1, **to(peer))
    for peer in (p1, p2, p3):
        pl.semaphore_signal(barrier, inc=1, **to_y(peer))
    pl.semaphore_wait(barrier, 6)

    for h in range(2):
        for n in range(3):
            own_send(n, h, 0).start()
    for copy in locals_:
        copy.start()

    kv_wide = kv_heads * head
    gbuf[...] = jnp.zeros(gbuf.shape, F32)
    gbuf[0:heads, 0:head] = qgain_ref[...].astype(F32)
    gbuf[heads:heads + kv_heads, 0:head] = kgain_ref[...].astype(F32)
    gain_t = jnp.transpose(gbuf[...])
    gswap_t = swap_pairs(gain_t)
    line = lax.broadcasted_iota(jnp.int32, (head, rb), 0)
    odd = lax.rem(line, 2)
    inv_freq = jnp.exp((line - odd).astype(F32) * (-math.log(ROPE_THETA) / head))
    angles = inv_freq * pos_ref[...].astype(F32)
    cos_a = jnp.cos(angles)
    sin_a = jnp.sin(angles) * (2 * odd - 1).astype(F32)
    qkv_copy.wait()
    qkv_t = jnp.transpose(qkv_ref[...].astype(F32))
    swap_t = swap_pairs(qkv_t[:natt + kv_wide])
    for n in range(heads + kv_heads):
        own = slice(n * head, (n + 1) * head)
        one, two = qkv_t[own], swap_t[own]
        mean = jnp.mean(one, axis=0, keepdims=True)
        centred = one - mean
        scale = lax.rsqrt(jnp.mean(centred * centred, axis=0, keepdims=True) + NORM_EPS)
        turned = (centred * scale * gain_t[:head, n:n + 1] * cos_a
                  + (two - mean) * scale * gswap_t[:head, n:n + 1] * sin_a)
        turned = turned.astype(BF16)
        if n < heads:
            qt[n] = turned.astype(F32)
        else:
            k_out[n - heads] = turned
            kt[n - heads] = turned.astype(F32)
    for n in range(kv_heads):
        one = qkv_t[natt + kv_wide + n * head:natt + kv_wide + (n + 1) * head]
        vt[n] = one
        v_out[n] = one.astype(BF16)

    new_leave = (pltpu.make_async_copy(k_out, k_hbm, o_sem.at[0]), pltpu.make_async_copy(v_out, v_hbm, o_sem.at[1]))
    for copy in new_leave:
        copy.start()

    score_scale = head ** -0.5
    db = 16

    def attend_head(kv, carry):
        first = kv * group

        def score_chunk(c, inner):
            idx = kv * n_chunks + c
            slot = lax.rem(idx, 2)
            cache_copy(0, idx).wait()

            @pl.when(idx < kv_heads * n_chunks - 1)
            def _():
                cache_copy(0, idx + 1).start()

            def score(s, deep):
                keys = kbuf[slot, s].astype(F32)
                sc[c * cs + s] = jnp.concatenate(
                    [jnp.sum(qt[first + j] * keys, axis=0, keepdims=True) for j in range(group)], axis=0)
                return deep

            return lax.fori_loop(0, cs, score, inner)

        lax.fori_loop(0, n_chunks, score_chunk, 0)
        k_one = kt[kv]
        s_one = jnp.concatenate([jnp.sum(qt[first + j] * k_one, axis=0, keepdims=True) for j in range(group)], axis=0) * score_scale
        scores = sc[...] * score_scale
        at = lax.broadcasted_iota(jnp.int32, scores.shape, 0)
        scores = jnp.where(at < pos_ref[...][None], scores, -1e30)
        top = jnp.maximum(jnp.max(scores, axis=0), s_one)
        probs = jnp.exp(scores - top[None])
        p_one = jnp.exp(s_one - top)
        denom = jnp.sum(probs, axis=0) + p_one
        sc[...] = probs.astype(BF16).astype(F32)
        v_one = vt[kv]
        for j in range(group):
            oc[j] = p_one[j:j + 1] * v_one

        def value_chunk(c, inner):
            idx = kv * n_chunks + c
            slot = lax.rem(idx, 2)
            cache_copy(1, idx).wait()

            @pl.when(idx < kv_heads * n_chunks - 1)
            def _():
                cache_copy(1, idx + 1).start()

            def value(b, deep):
                lines = pl.ds(pl.multiple_of(b * db, db), db)
                sums = [oc[j, lines, :] for j in range(group)]
                for s in range(cs):
                    vals = vbuf[slot, s, lines, :].astype(F32)
                    for j in range(group):
                        sums[j] = sums[j] + sc[c * cs + s, j:j + 1, :] * vals
                for j in range(group):
                    oc[j, lines, :] = sums[j]
                return deep

            return lax.fori_loop(0, head // db, value, inner)

        lax.fori_loop(0, n_chunks, value_chunk, 0)
        for j in range(group):
            lines = pl.ds(pl.multiple_of((first + j) * head, 8), head)
            ot[lines, :] = oc[j] / denom[j:j + 1]
        return carry

    lax.fori_loop(0, kv_heads, attend_head, 0)
    gath[0, :, 0:natt] = jnp.transpose(ot[...]).astype(BF16)
    for h in range(2):
        for n in range(3):
            own_send(n, h, 1).start()
    for copy in locals_:
        copy.wait()

    def block_rows(place, j):
        off = place + (place // 2) * (5 - 2 * place)
        who = core + j * (1 - 2 * core)
        return (lax.rem(xi + off, nx) * 2 + who) * rb

    groups = [(place, 0, rb) for place in range(nx - 1)] + [(nx - 1, 0, hb), (nx - 1, hb, hb)]

    def aligned(start, size):
        return pl.ds(pl.multiple_of(start, size), size)

    def y1(g, j):
        place, row0, size = groups[g]
        i = 2 * place + j
        return pltpu.make_async_remote_copy(
            src_ref=pb.at[i, aligned(row0 + (1 - b1) * (size // 2), size // 2), :], dst_ref=r1.at[i, pl.ds(row0 // 2, size // 2), :],
            send_sem=y1s.at[2 * g + j], recv_sem=y1r.at[2 * g + j], **to_y(p1))

    def y2(g, j):
        place, row0, size = groups[g]
        i = 2 * place + j
        rows = pl.ds(row0 // 4, size // 4)
        return pltpu.make_async_remote_copy(
            src_ref=mq.at[i, rows, :], dst_ref=r2.at[i, rows, :],
            send_sem=y2s.at[2 * g + j], recv_sem=y2r.at[2 * g + j], **to_y(p2))

    def y3(g, j, mine):
        place, row0, size = groups[g]
        quarter = b2 if mine else 1 - b2
        start = block_rows(place, j) + row0 + b1 * (size // 2) + quarter * (size // 4)
        rows = out_ref.at[aligned(start, size // 4), :]
        return pltpu.make_async_remote_copy(
            src_ref=rows, dst_ref=rows, send_sem=y3s.at[2 * g + j], recv_sem=y3r.at[2 * g + j], **to_y(p2))

    last = len(groups) - 1

    def y4(g, j, mine):
        place, row0, size = groups[g]
        start = block_rows(place, j) + row0 + (b1 if mine else 1 - b1) * (size // 2)
        count = size // 2
        if g == last:
            start = start + (b2 if mine else q1) * (size // 4)
            count = size // 4
        rows = out_ref.at[aligned(start, count), :]
        return pltpu.make_async_remote_copy(
            src_ref=rows, dst_ref=rows, send_sem=y4s.at[2 * g + j], recv_sem=y4r.at[2 * g + j], **to_y(p1))

    def y5(j, mine):
        place, row0, size = groups[last]
        start = block_rows(place, j) + row0 + (b1 if mine else 1 - b1) * (size // 2) + (b2 if mine else 1 - q1) * (size // 4)
        rows = out_ref.at[aligned(start, size // 4), :]
        return pltpu.make_async_remote_copy(
            src_ref=rows, dst_ref=rows, send_sem=y5s.at[j], recv_sem=y5r.at[j], **to_y(p3))

    def product(g, kinds=(0, 1)):
        place, row0, size = groups[g]
        rows = pl.ds(row0, size)
        if len(kinds) == 2:
            cols = slice(None)
        else:
            cols = att_cols if kinds[0] else act_cols

        def body(j, carry):
            i = 2 * place + j

            @pl.when(j == 1)
            def _():
                for kind in kinds:
                    for h in range(row0 // hb, (row0 + size) // hb):
                        landed(2 * place + 1, h, kind).wait_recv()

            part = jnp.dot(gath[i, rows, cols], w2[cols, :], preferred_element_type=F32)
            if kinds == (1,):
                part = part + mf[i, rows, :]
            mf[i, rows, :] = part
            if 1 in kinds:
                pb[i, rows, :] = part.astype(BF16)
                y1(g, j).start()
            return carry

        lax.fori_loop(0, 2, body, 0)

    def stage2(g):
        place, row0, size = groups[g]
        for j in range(2):
            i = 2 * place + j
            y1(g, j).wait_recv()
            rows = aligned(row0 + b1 * (size // 2) + (1 - b2) * (size // 4), size // 4)
            sub = aligned(row0 // 2 + (1 - b2) * (size // 4), size // 4)
            mq[i, row0 // 4:(row0 + size) // 4, :] = (mf[i, rows, :] + r1[i, sub, :].astype(F32)).astype(BF16)
            y2(g, j).start()

    def stage3(g):
        place, row0, size = groups[g]
        for j in range(2):
            i = 2 * place + j
            y2(g, j).wait_recv()
            rows = aligned(row0 + b1 * (size // 2) + b2 * (size // 4), size // 4)
            sub = aligned(row0 // 2 + b2 * (size // 4), size // 4)
            total = mf[i, rows, :] + r1[i, sub, :].astype(F32) + r2[i, row0 // 4:(row0 + size) // 4, :].astype(F32)
            rows = aligned(block_rows(place, j) + row0 + b1 * (size // 2) + b2 * (size // 4), size // 4)
            out_ref[rows, :] = (x_ref[rows, :].astype(F32) + total).astype(BF16)
            y3(g, j, True).start()
            if g == last:
                y5(j, True).start()
                y4(g, j, True).start()

    def stage4(g):
        for j in range(2):
            y3(g, j, False).wait_recv()
            y4(g, j, True).start()

    def leave(g, j):
        place, row0, size = groups[g]
        rows = aligned(block_rows(place, j) + row0, size)
        return pltpu.make_async_copy(out_ref.at[rows, :], out_hbm.at[rows, :], o_sem.at[2 + 2 * g + j])

    def settled(g):
        for j in range(2):
            if g == last:
                y3(g, j, False).wait_recv()
                y5(j, False).wait_recv()
            y4(g, j, False).wait_recv()
            leave(g, j).start()

    def near_landed(kind):
        for slot in (2, 4):
            for h in range(2):
                landed(slot, h, kind).wait_recv()
        if kind == 0:
            forwards = ((0, 0),)
        else:
            forwards = ((0, 1), (1, 0), (1, 1))
        for h, k in forwards:
            for n in range(2):
                opp_send(n, h, k).start()
        for slot in (2, 4):
            for h in range(2):
                par_send(slot, h, kind).start()

    def far_landed(h, kind):
        for n in range(2):
            opp_landed(n, h, kind).wait_recv()
        par_send(6, h, kind).start()

    product(0)
    stage2(0)
    near_landed(0)
    stage3(0)
    near_landed(1)
    stage4(0)
    product(1)
    product(2)
    stage2(1)
    stage2(2)
    far_landed(0, 0)
    far_landed(0, 1)
    stage3(1)
    stage3(2)
    product(3)
    stage4(1)
    stage4(2)
    stage2(3)
    far_landed(1, 0)
    stage3(3)
    product(4, (0,))
    for g in range(nx - 1):
        settled(g)
    far_landed(1, 1)
    product(4, (1,))
    stage4(3)
    stage2(4)
    stage3(4)

    for g in range(nx - 1, len(groups)):
        settled(g)
    for g in range(len(groups)):
        for j in range(2):
            leave(g, j).wait()
            y1(g, j).wait_send()
            y2(g, j).wait_send()
            y3(g, j, True).wait_send()
            y4(g, j, True).wait_send()
    for j in range(2):
        y5(j, True).wait_send()
    for copy in new_leave:
        copy.wait()
    for kind in range(2):
        for h in range(2):
            for n in range(3):
                own_send(n, h, kind).wait_send()
            for slot in (2, 4, 6):
                par_send(slot, h, kind).wait_send()
            for n in range(2):
                opp_send(n, h, kind).wait_send()


def finish(nx, ny, act, qkv, k_cache, v_cache, positions, q_gain, k_gain, w_out, w_down, x_in):
    rb, nf = act.shape
    kv_heads, ctx, head = k_cache.shape[:3]
    natt, wcols = w_out.shape
    heads = natt // head
    group = heads // kv_heads
    cs = 16
    vmem = pl.BlockSpec(memory_space=pltpu.VMEM)
    hbm = pl.BlockSpec(memory_space=ANY)
    dma = pltpu.SemaphoreType.DMA
    new = jax.ShapeDtypeStruct((kv_heads, head, rb), BF16)
    return pl.pallas_call(
        functools.partial(finish_kernel, nx, ny, heads, kv_heads),
        out_shape=(jax.ShapeDtypeStruct(x_in.shape, BF16), new, new),
        in_specs=[hbm, hbm, hbm, hbm, vmem, vmem, vmem, hbm, hbm, hbm],
        out_specs=(hbm, hbm, hbm),
        scratch_shapes=[
            pltpu.VMEM(x_in.shape, BF16),
            pltpu.VMEM(new.shape, BF16),
            pltpu.VMEM(new.shape, BF16),
            dma((2 + 4 * nx,)),
            pltpu.VMEM(qkv.shape, BF16),
            pltpu.VMEM(x_in.shape, BF16),
            pltpu.VMEM((128, pl.cdiv(head, 128) * 128), F32),
            pltpu.VMEM((2 * nx, rb, natt + nf), BF16),
            pltpu.VMEM((natt + nf, wcols), BF16),
            pltpu.VMEM((heads, head, rb), F32),
            pltpu.VMEM((kv_heads, head, rb), F32),
            pltpu.VMEM((kv_heads, head, rb), F32),
            pltpu.VMEM((ctx, group, rb), F32),
            pltpu.VMEM((group, head, rb), F32),
            pltpu.VMEM((natt, rb), F32),
            pltpu.VMEM((2, cs, head, rb), BF16),
            pltpu.VMEM((2, cs, head, rb), BF16),
            pltpu.VMEM((2 * nx, rb, wcols), BF16),
            pltpu.VMEM((2 * nx, rb // 2, wcols), BF16),
            pltpu.VMEM((2 * nx, rb, wcols), F32),
            pltpu.VMEM((2 * nx, rb // 4, wcols), BF16),
            pltpu.VMEM((2 * nx, rb // 4, wcols), BF16),
            dma((5,)),
            dma((2, 2)),
            dma((3, 2, 2)),
            dma((2, 2, 2)),
            dma((3, 2, 2)),
            dma((2 * nx + 1, 2, 2)),
        ] + [dma((2 * nx + 2,))] * 8 + [dma((2,))] * 2,
        compiler_params=pltpu.CompilerParams(collective_id=1, has_side_effects=True, vmem_limit_bytes=VMEM_LIMIT),
        name='finish',
    )(act, qkv, k_cache, v_cache, positions, q_gain, k_gain, w_out, w_down, x_in)


def settle_kernel(n_parts, x_ref, k_ref, v_ref, x_out, k_out, v_out, xbuf, kbuf, vbuf, sem_in, sem_out):
    rows = x_ref.shape[0] // n_parts
    moves = [(x_ref.at[pl.ds(n * rows, rows)], xbuf.at[pl.ds(n * rows, rows)], x_out.at[pl.ds(n * rows, rows)]) for n in range(n_parts)]
    moves += [(k_ref, kbuf, k_out), (v_ref, vbuf, v_out)]
    for n, (src, mid, _) in enumerate(moves):
        pltpu.make_async_copy(src, mid, sem_in.at[n]).start()
    for n, (src, mid, dst) in enumerate(moves):
        pltpu.make_async_copy(src, mid, sem_in.at[n]).wait()
        pltpu.make_async_copy(mid, dst, sem_out.at[n]).start()
    for n, (_, mid, dst) in enumerate(moves):
        pltpu.make_async_copy(mid, dst, sem_out.at[n]).wait()


def settle(x_out, k_t, v_t):
    n_parts = 4
    hbm = pl.BlockSpec(memory_space=ANY)
    arrays = (x_out, k_t, v_t)
    return pl.pallas_call(
        functools.partial(settle_kernel, n_parts),
        out_shape=tuple(jax.ShapeDtypeStruct(a.shape, a.dtype) for a in arrays),
        in_specs=[hbm] * 3,
        out_specs=(hbm,) * 3,
        scratch_shapes=[pltpu.VMEM(a.shape, a.dtype) for a in arrays] + [pltpu.SemaphoreType.DMA((n_parts + 2,))] * 2,
        name='settle',
    )(*arrays)


def solution(mesh):
    dm_size = mesh.shape['dm']
    nx = dm_size // 2
    x_spec = P('dp', 'dm')
    row_spec = P(('dp', 'dm'))
    cache_spec = P(('dp', 'dm'), 'tp', None, None)
    new_spec = P(('dp', 'dm'), 'tp', None)
    hid_tp = P('dm', 'tp')
    tp_hid = P('tp', 'dm')
    head_spec = P('tp', None)

    def device_step(x_in, positions, k_cache, v_cache, ln_gain, w_q, w_k, w_v, w_gate, w_up, q_gain, k_gain, w_out, w_down):
        qkv, act = project(nx, x_in, ln_gain, w_q, w_k.T, w_v.T, w_gate, w_up)
        x_out, k_t, v_t = settle(*finish(
            nx, mesh.shape['tp'], act, qkv, jnp.transpose(k_cache, (1, 2, 3, 0)), jnp.transpose(v_cache, (1, 2, 3, 0)),
            positions[None, :], q_gain, k_gain, w_out, w_down, x_in))
        k_new = jnp.transpose(k_t, (2, 0, 1))
        v_new = jnp.transpose(v_t, (2, 0, 1))
        return x_out, k_new, v_new

    return jax.shard_map(
        device_step,
        mesh=mesh,
        in_specs=(x_spec, row_spec, cache_spec, cache_spec, P('dm'), hid_tp, hid_tp, hid_tp, hid_tp, hid_tp, head_spec, head_spec, tp_hid, tp_hid),
        out_specs=(x_spec, new_spec, new_spec),
        check_vma=False,
    )
```
